512 devices in a mesh: grp: 2 (over y), sp: 16 (over z), sub: 8 (over x), rep: 2 (over core).
Axes of the slice: x: 8, y: 2, z: 16, core: 2. Of those that a mesh axis runs over, the one named last changes fastest.
The devices are a block of a 8x8x16 slice.
Arguments:
- field: float32 [512, 32, 32, 128], P(('grp', 'sp', 'rep'), 'sub'), parts along dimension 0, may hold values from -40 to 40, as said below
- mix_weight: float32 [256, 256], replicated, may hold values from -0.375 to 0.375
- factor_x: float32 [256, 32], replicated, may hold values from -6 to 6
- factor_y: float32 [256, 32], replicated, may hold values from -6 to 6
- factor_z: float32 [256, 32], replicated, may hold values from -6 to 6
- norm_gain: float32 [256], replicated, may hold values from 0.5 to 1.5
- norm_bias: float32 [256], replicated, may hold values from -3 to 3
- w_in: float32 [256, 256], replicated, may hold values from -0.375 to 0.375
- b_in: float32 [256], replicated, may hold values from -3 to 3
- w_out: float32 [256, 256], replicated, may hold values from -0.375 to 0.375
- b_out: float32 [256], replicated, may hold values from -3 to 3
Outputs:
- block_out: float32 [512, 32, 32, 128], P('grp', 'sub', ('sp', 'rep')), parts along dimension 0
The draws below stay inside these ranges and needn't reach their ends.
There are 2 independent parts, one for each index of `grp`. The reference program is written for one: setup_inputs(seed, part) draws one part's arguments, and reference() takes and returns one part's arrays. A program takes and returns all parts, laid end to end along the dimension named above; an argument that names none is the same for every part. Nothing has to cross between parts.
Inputs may be any that keep to these rules, and one draw needn't show every extreme that they name: `field`: real values of order one in each channel, with scales that differ between channels.
All inputs are finite; a program needn't handle non-finite values.
Results may differ from the reference program's by a relative error of at most 0.000078.
Values sent between devices are 32-bit elements; how exact they have to be, the bound alone decides.
A program may use at most 64 MiB of HBM per device.

```python
import math
import jax
import jax.numpy as jnp
from jax import lax

C = 256
HID = 256
KX = 32
KY = 32
KZ = 32
GROUPS = 32
NX = 32
NY = 32
NZ = 128


def draw_field(key, part):
    first, second = jax.random.split(key, 2)
    chan_scale = jnp.exp(jax.random.uniform(second, (C, 1, 1, 1), jnp.float32, math.log(0.3), math.log(3.0)))
    along_x = jnp.arange(NX, dtype=jnp.float32) / (NX - 1)
    along_y = jnp.arange(NY, dtype=jnp.float32) / (NY - 1)
    ramp = jnp.exp(math.log(3.0) * (along_x[:, None, None] + along_y[None, :, None]) - math.log(3.0))
    base = jnp.clip(jax.random.normal(first, (C, NX, NY, NZ), jnp.float32), -4.0, 4.0)
    return base * chan_scale * ramp[None]


def noise(own_key, shape, spread, reach, kind=jnp.bfloat16):
    drawn = jax.random.normal(own_key, shape, jnp.float32) * spread
    return jnp.minimum(jnp.maximum(drawn, -reach), reach).astype(kind)


def setup_inputs(seed: int = 0, part: int = 0) -> dict:
    splits = jax.random.split(jax.random.key(seed), 12)
    part_splits = jax.random.split(jax.random.fold_in(splits[11], part), 12)
    field = draw_field(jax.random.fold_in(jax.random.fold_in(splits[11], part), 71), part)
    mix_weight = noise(splits[1], (C, C), C ** -0.5, 0.375, jnp.float32)
    factor_x = noise(splits[2], (C, KX), 1.3, 6.0, jnp.float32)
    factor_y = noise(splits[3], (C, KY), 1.3, 6.0, jnp.float32)
    factor_z = noise(splits[4], (C, KZ), 1.3, 6.0, jnp.float32)
    norm_gain = jnp.clip(jax.random.uniform(splits[5], (C,), jnp.float32, 0.5, 1.5), 0.5, 1.5)
    norm_bias = noise(splits[6], (C,), 0.5, 3.0, jnp.float32)
    w_in = noise(splits[7], (HID, C), C ** -0.5, 0.375, jnp.float32)
    b_in = noise(splits[8], (HID,), 0.5, 3.0, jnp.float32)
    w_out = noise(splits[9], (C, HID), HID ** -0.5, 0.375, jnp.float32)
    b_out = noise(splits[10], (C,), 0.5, 3.0, jnp.float32)
    return dict(field=field, mix_weight=mix_weight, factor_x=factor_x, factor_y=factor_y, factor_z=factor_z, norm_gain=norm_gain, norm_bias=norm_bias, w_in=w_in, b_in=b_in, w_out=w_out, b_out=b_out)


def contract(formula, left, right):
    return jnp.einsum(formula, left, right, precision=lax.Precision.HIGHEST)

def tables(length, kept_count):
    indices = jnp.arange(kept_count, dtype=jnp.int32)
    kept_freq = jnp.where(indices < kept_count // 2, indices, length - kept_count + indices)
    positions = jnp.arange(length, dtype=jnp.int32)
    phases = kept_freq[:, None] * positions[None, :] % length
    angles = 2.0 * math.pi / length * phases.astype(jnp.float32)
    return (jnp.cos(angles), jnp.sin(angles))

def transform(planes, cosine, sine, formula):
    real_part = contract(formula, planes[0], cosine) + contract(formula, planes[1], sine)
    imag_part = contract(formula, planes[1], cosine) - contract(formula, planes[0], sine)
    return jnp.stack([real_part, imag_part])

def reference(field, mix_weight, factor_x, factor_y, factor_z, norm_gain, norm_bias, w_in, b_in, w_out, b_out):
    cos_x, sin_x = tables(NX, KX)
    cos_y, sin_y = tables(NY, KY)
    cos_z, sin_z = tables(NZ, KZ)
    planes = jnp.stack([contract('cxyz,kz->cxyk', field, cos_z / NZ), -contract('cxyz,kz->cxyk', field, sin_z / NZ)])
    planes = transform(planes, cos_y / NY, sin_y / NY, 'cxyk,jy->cxjk')
    spectra = transform(planes, cos_x / NX, sin_x / NX, 'cxjk,ix->cijk')
    weighting = factor_x[:, :, None, None] * factor_y[:, None, :, None] * factor_z[:, None, None, :]
    mixed_modes = jnp.einsum('oc,rcijk->roijk', mix_weight, spectra * weighting[None], precision=lax.Precision.HIGHEST)
    returned = transform(mixed_modes, cos_x, -sin_x, 'cijk,ix->cxjk')
    returned = transform(returned, cos_y, -sin_y, 'cxjk,jy->cxyk')
    spectral = contract('cxyk,kz->cxyz', returned[0], cos_z) - contract('cxyk,kz->cxyz', returned[1], sin_z)
    summed = field + spectral
    cells_group = C // GROUPS * NX * NY * NZ
    grouped = summed.reshape(GROUPS, -1)
    group_mean = lax.optimization_barrier(jnp.sum(grouped, axis=1)) / cells_group
    centered = grouped - group_mean[:, None]
    group_var = lax.optimization_barrier(jnp.sum(centered * centered, axis=1)) / cells_group
    inv_scale = jnp.repeat(lax.rsqrt(group_var + 1e-05), C // GROUPS) * norm_gain
    mean_chan = jnp.repeat(group_mean, C // GROUPS)
    columns = summed.reshape(C, -1)
    normed = (columns - mean_chan[:, None]) * inv_scale[:, None] + norm_bias[:, None]
    hidden = jax.nn.gelu(jnp.dot(w_in, normed, precision=lax.Precision.HIGHEST) + b_in[:, None])
    result = columns + jnp.dot(w_out, hidden, precision=lax.Precision.HIGHEST) + b_out[:, None]
    return result.reshape(C, NX, NY, NZ)
```

```python
import math

import jax
import jax.numpy as jnp
import numpy as np
from jax import lax
from jax.experimental import pallas as pl
from jax.experimental.pallas import tpu as pltpu
from jax.sharding import PartitionSpec as P

F32 = jnp.float32
BF16 = jnp.bfloat16
GROUP_CHANNELS = 8
EPS = 1e-05


def split_np(a):
    a = np.asarray(a, np.float32)
    hi = a.astype(BF16)
    lo = (a - hi.astype(np.float32)).astype(BF16)
    return hi, lo


def build_tables(nx, ny, nz, kz, ch_local, wide):
    xl = 4
    chunks = 8
    lane = np.arange(128)
    k_of, x_of, r_of = lane // 16, (lane // 4) % 4, lane % 4
    z = np.arange(nz)
    scale = 1.0 / (nx * ny * nz)
    top = kz // 2
    fwd_z = np.zeros((xl, nz, 256))
    inv_z = np.zeros((256, xl, nz))
    for l in range(128):
        f = 2 * k_of[l] + r_of[l] // 2
        ang = 2 * np.pi * ((f * z) % nz) / nz
        fwd_z[x_of[l], :, l] = (np.cos(ang) if r_of[l] % 2 == 0 else -np.sin(ang)) * scale
        inv_z[l, x_of[l], :] = np.cos(ang) if r_of[l] % 2 == 0 else -np.sin(ang)
        if r_of[l] < 2:
            ang = 2 * np.pi * ((top * z) % nz) / nz
            col = np.cos(ang) if r_of[l] == 0 else -np.sin(ang)
            fwd_z[x_of[l], :, 128 + l] = col * scale
            inv_z[128 + l, x_of[l], :] = col
    fwd_z = fwd_z.reshape(xl * nz, 256)
    inv_z = inv_z.reshape(256, xl * nz)
    ax = np.arange(nx)
    ang = 2 * np.pi * ((ax[:, None] * ax[None, :]) % nx) / nx
    c, s = np.cos(ang), np.sin(ang)
    fwd = np.zeros((nx, 2, 2, nx, 2, 2))
    inv = np.zeros((nx, 2, 2, nx, 2, 2))
    for f in range(2):
        fwd[:, f, 0, :, f, 0] = c
        fwd[:, f, 1, :, f, 0] = s
        fwd[:, f, 0, :, f, 1] = -s
        fwd[:, f, 1, :, f, 1] = c
        inv[:, f, 0, :, f, 0] = c
        inv[:, f, 1, :, f, 0] = -s
        inv[:, f, 0, :, f, 1] = s
        inv[:, f, 1, :, f, 1] = c
    turn = np.zeros((128, 128))
    for l in range(0, 128, 2):
        turn[l + 1, l] = 1.0
        turn[l, l + 1] = -1.0
    fwd = fwd.reshape(128, 128)
    inv = inv.reshape(128, 128)
    x_fwd = np.concatenate([fwd, fwd @ turn], 1)
    x_inv = np.concatenate([inv, -(inv @ turn)], 1)
    ay = np.arange(ny)
    ang = 2 * np.pi * ((ay[:, None] * ay[None, :]) % ny) / ny
    y_tab = np.concatenate([np.cos(ang), np.sin(ang)], 1)
    hi, lo = split_np(y_tab)
    y_tab3 = np.concatenate([hi, hi, lo], 1)
    sel_x = np.zeros((nx, 256))
    for a in range(nx):
        sel_x[a, 4 * a : 4 * a + 4] = 1.0
        sel_x[a, 128 + 4 * ((nx - a) % nx) : 128 + 4 * ((nx - a) % nx) + 4] = 1.0
    sel_z = np.zeros((kz, 2, 9, nx, 4))
    for f in range(top + 1):
        k, f2 = f // 2, f % 2
        if f < top:
            sel_z[f, 0, k, :, 2 * f2 : 2 * f2 + 2] = 1.0
        if f > 0:
            sel_z[kz - f, 1, k, :, 2 * f2 : 2 * f2 + 2] = 1.0
    sel_z = sel_z.reshape(kz, 2 * 9 * 128)
    rows_in = np.arange(ch_local * ny)
    rows_out = np.arange(ch_local * 8)
    gather = (
        (rows_in[None, :] // ny == rows_out[:, None] // 8)
        & (rows_in[None, :] % 8 == rows_out[:, None] % 8)
    ).astype(np.float32)
    rows_all = np.arange(ch_local * wide)
    spread = (rows_all[:, None] // ch_local == np.arange(wide)[None, :]).astype(np.float32)
    fz = split_np(fwd_z)
    iz = split_np(inv_z)
    xf = split_np(x_fwd)
    xi = split_np(x_inv)
    return dict(
        fz_hi=fz[0], fz_lo=fz[1], iz_hi=iz[0], iz_lo=iz[1],
        xf_hi=xf[0], xf_lo=xf[1], xi_hi=xi[0], xi_lo=xi[1],
        y_tab=y_tab3,
        sel_x=sel_x.astype(np.float32), sel_z=sel_z.astype(np.float32),
        gather=gather.astype(BF16), spread=spread.astype(BF16),
    )


def split(a):
    hi = a.astype(BF16)
    return hi, (a - hi.astype(F32)).astype(BF16)


def dot1(a, b):
    return lax.dot_general(a, b, (((1,), (0,)), ((), ())), preferred_element_type=F32)


def dot3(a, b):
    return dot1(a[0], b[0]) + dot1(a[0], b[1]) + dot1(a[1], b[0])


def exact(a, b):
    return lax.dot_general(
        a, b, (((1,), (0,)), ((), ())), precision=lax.Precision.HIGHEST, preferred_element_type=F32
    )


def swap_chunks(arrays, roll):
    arrays = list(arrays)
    rows = arrays[0].shape[0]
    chunk = lax.broadcasted_iota(jnp.int32, (rows, 128), 1) // 16
    for d in (4, 2, 1):
        upper = (chunk // d) % 2 == 1
        for i in range(8):
            if (i // d) % 2 == 0:
                low, high = arrays[i], arrays[i + d]
                arrays[i] = jnp.where(upper, roll(high, 16 * d), low)
                arrays[i + d] = jnp.where(upper, high, roll(low, 128 - 16 * d))
    return arrays


def forward_z(parts, tabs):
    fz_hi, fz_lo = tabs["fz_hi"], tabs["fz_lo"]
    total = None
    for x, part in enumerate(parts):
        term = dot3(split(part), (fz_hi[128 * x : 128 * x + 128], fz_lo[128 * x : 128 * x + 128]))
        total = term if total is None else total + term
    main, extra = total[:, :128], total[:, 128:]
    rows, lanes = (lax.broadcasted_iota(jnp.int32, extra.shape, d) for d in (0, 1))
    extra = jnp.where((rows % 32) // 8 == lanes // 16, extra, 0.0)
    hi, lo = split(extra)
    packed = dot1(tabs["gather"], hi) + dot1(tabs["gather"], lo)
    return main, packed


def factor_weights(row_x, row_y, row_z, tabs):
    lanes_x = exact(row_x, tabs["sel_x"])
    lanes_z = exact(row_z, tabs["sel_z"])
    plus = lanes_z[:, :1152] * jnp.concatenate([lanes_x[:, :128]] * 9, 1)
    minus = lanes_z[:, 1152:] * jnp.concatenate([lanes_x[:, 128:]] * 9, 1)
    n = row_y.shape[1]
    r, c = (lax.broadcasted_iota(jnp.int32, (n, n), d) for d in (0, 1))
    wide = jnp.broadcast_to(row_y, (n, n))
    col_plus = jnp.sum(jnp.where(r == c, wide, 0.0), axis=1, keepdims=True)
    col_minus = jnp.sum(jnp.where((n - r) % n == c, wide, 0.0), axis=1, keepdims=True)
    return col_plus * plus + col_minus * minus


def spectral_filter(blocks, weights, tabs, roll):
    main = swap_chunks([b[:32] for b in blocks], roll)
    extra = swap_chunks([b[32:40] for b in blocks], roll)
    last = jnp.concatenate(extra[:4], 0)
    rows = jnp.concatenate(main + [last], 0)

    def along_y(pairs):
        stacked = jnp.concatenate(
            [
                jnp.concatenate(
                    [pairs[32 * k : 32 * k + 32, :128], pairs[32 * k : 32 * k + 32, 128:]], 0
                )
                for k in range(9)
            ],
            1,
        )
        hi, lo = split(stacked)
        return dot1(tabs["y_tab"], jnp.concatenate([hi, lo, hi], 0))

    pairs = dot3(split(rows), (tabs["xf_hi"], tabs["xf_lo"]))
    spec = along_y(pairs) * weights
    rows = jnp.concatenate([spec[:, 128 * k : 128 * k + 128] for k in range(9)], 0)
    pairs = dot3(split(rows), (tabs["xi_hi"], tabs["xi_lo"]))
    back = along_y(pairs)
    main = swap_chunks([back[:, 128 * k : 128 * k + 128] for k in range(8)], roll)
    last = back[:, 1024:]
    tiles = [last[8 * p : 8 * p + 8] for p in range(4)] + [jnp.zeros((8, 128), F32)] * 4
    extra = swap_chunks(tiles, roll)
    return main, extra


def leftover_rows(extras, roll):
    return jnp.concatenate(swap_chunks(extras, roll)[:4], 0)


def inverse_z(modes, left, mix, tabs):
    hi, lo = split(left)
    wide = dot1(tabs["spread"], hi) + dot1(tabs["spread"], lo)
    rows, lanes = (lax.broadcasted_iota(jnp.int32, wide.shape, d) for d in (0, 1))
    wide = jnp.where(rows % 8 == lanes // 16, wide, 0.0)
    both = jnp.concatenate([modes, wide], 1)
    mixed = dot3(mix, split(both))
    return dot3(split(mixed), (tabs["iz_hi"], tabs["iz_lo"]))


def to_column(row):
    n = row.shape[1]
    r, c = (lax.broadcasted_iota(jnp.int32, (n, n), d) for d in (0, 1))
    return jnp.sum(jnp.where(r == c, jnp.broadcast_to(row, (n, n)), 0.0), axis=1, keepdims=True)


def group_partials(total):
    folded = jnp.sum(total.reshape(total.shape[0] // 8, 8, 128), axis=1)
    return jnp.sum(folded, axis=1, keepdims=True)


def stats_row(first, second):
    n = first.shape[0]
    r, c = (lax.broadcasted_iota(jnp.int32, (n, 128), d) for d in (0, 1))
    placed = jnp.where(r == c, first, 0.0) + jnp.where(r + n == c, second, 0.0)
    return jnp.sum(placed, axis=0, keepdims=True)


def stats_columns(row, count, channels):
    groups = channels // GROUP_CHANNELS
    r, c = (lax.broadcasted_iota(jnp.int32, (channels, 128), d) for d in (0, 1))
    wide = jnp.broadcast_to(row, (channels, 128))
    first = jnp.sum(jnp.where(r // GROUP_CHANNELS == c, wide, 0.0), axis=1, keepdims=True)
    second = jnp.sum(
        jnp.where(r // GROUP_CHANNELS + groups == c, wide, 0.0), axis=1, keepdims=True
    )
    mean = first / count
    var = second / count - mean * mean
    return mean, lax.rsqrt(var + EPS)


def gelu(v):
    inner = math.sqrt(2.0 / math.pi) * (v + 0.044715 * (v * v * v))
    return 0.5 * v * (1.0 + jnp.tanh(inner))


TABLES = (
    "fz_hi", "fz_lo", "iz_hi", "iz_lo", "xf_hi", "xf_lo", "xi_hi", "xi_lo",
    "y_tab", "sel_x", "sel_z", "gather", "spread",
)
MSG = 40


class Lazy:
    def __init__(self, refs):
        self.refs = refs

    def __getitem__(self, name):
        return self.refs[name][...]


def lane_roll(a, shift):
    return pltpu.roll(a, shift, axis=1)


def fused(sizes, *refs):
    wide, narrow, channels = sizes["wide"], sizes["narrow"], sizes["channels"]
    rep = sizes["rep"]
    (field, fac_x, fac_y, fac_z, mix, gain, bias, w_in, b_in, w_out, b_out) = refs[:11]
    tabs = Lazy(dict(zip(TABLES, refs[11 : 11 + len(TABLES)])))
    out = refs[11 + len(TABLES)]
    (
        src, fld, b1, r1, b2, r2, s3, n3, s3l, n3l, st0, ar1, st1, ar2,
        wts, mix_hi, mix_lo, in_hi, in_lo, out_hi, out_lo, cols, summed, send, recv,
    ) = refs[12 + len(TABLES) :]
    me_x = lax.axis_index("sub")
    me_z = lax.axis_index(("sp", "rep"))
    channel = me_z * narrow + me_x

    def z_id(q):
        return {"sp": q // rep, "rep": q % rep}

    def x_id(s):
        return {"sub": s}

    def z_peer(j):
        step = jnp.where(j % 2 == 1, (j + 1) // 2, wide - j // 2)
        return (me_z + step) % wide

    def x_peer(j):
        return (me_x + j) % narrow

    def push(a, b, slot, where):
        pltpu.make_async_remote_copy(
            src_ref=a, dst_ref=b, send_sem=send.at[slot], recv_sem=recv.at[slot],
            device_id=where, device_id_type=pl.DeviceIdType.MESH,
        ).start()

    def drain(ref, sem):
        pltpu.make_async_copy(ref, ref, sem).wait()

    def rows(start, size):
        return pl.ds(pl.multiple_of(start, 8), size)

    barrier = pltpu.get_barrier_semaphore()

    @pl.loop(1, narrow)
    def _(j):
        pl.semaphore_signal(
            barrier, inc=1, device_id=x_id(x_peer(j)), device_id_type=pl.DeviceIdType.MESH
        )

    @pl.loop(1, wide)
    def _(j):
        pl.semaphore_signal(
            barrier, inc=1, device_id=z_id(z_peer(j)), device_id_type=pl.DeviceIdType.MESH
        )

    parts = [
        jnp.concatenate([field[128 * c + 32 * x : 128 * c + 32 * x + 32] for c in range(8)], 0)
        for x in range(4)
    ]
    main, packed = forward_z(parts, tabs)
    for c in range(8):
        b1[MSG * c : MSG * c + 32] = main[32 * c : 32 * c + 32]
        b1[MSG * c + 32 : MSG * c + 40] = packed[8 * c : 8 * c + 8]
    for y in range(32):
        src[32 * y : 32 * y + 32] = field[pl.ds(y, 32, stride=32)]

    pl.semaphore_wait(barrier, narrow - 1 + wide - 1)

    @pl.loop(1, narrow)
    def _(j):
        s = x_peer(j)
        push(b1.at[rows(s * MSG, MSG)], r1.at[rows(me_x * MSG, MSG)], 0, x_id(s))

    @pl.loop(1, wide)
    def _(j):
        q = z_peer(j)
        push(src.at[rows(q * 32, 32)], fld.at[rows(me_z * 32, 32)], 1, z_id(q))

    r1[rows(me_x * MSG, MSG)] = b1[rows(me_x * MSG, MSG)]
    fld[rows(me_z * 32, 32)] = src[rows(me_z * 32, 32)]
    one = pl.ds(channel, 1)
    wts[...] = factor_weights(fac_x[one, :], fac_y[one, :], fac_z[one, :], tabs)
    for full, hi, lo in ((mix, mix_hi, mix_lo), (w_in, in_hi, in_lo), (w_out, out_hi, out_lo)):
        hi[...], lo[...] = split(full[...])
    for n, row in enumerate((gain, bias, b_in, b_out)):
        cols[n] = jnp.broadcast_to(to_column(row[...]), (channels, 128))

    drain(r1.at[pl.ds(0, MSG * (narrow - 1))], recv.at[0])
    blocks = [r1[MSG * s : MSG * s + MSG] for s in range(8)]
    main, extra = spectral_filter(blocks, wts[...], tabs, lane_roll)
    for s in range(8):
        b2[MSG * s : MSG * s + 32] = main[s]
        b2[MSG * s + 32 : MSG * s + 40] = extra[s]

    @pl.loop(1, narrow)
    def _(j):
        s = x_peer(j)
        push(b2.at[rows(s * MSG, MSG)], r2.at[rows(me_x * MSG, MSG)], 2, x_id(s))

    r2[rows(me_x * MSG, MSG)] = b2[rows(me_x * MSG, MSG)]
    drain(r2.at[pl.ds(0, MSG * (narrow - 1))], recv.at[2])
    left = leftover_rows([r2[MSG * c + 32 : MSG * c + 40] for c in range(8)], lane_roll)
    for y in range(32):
        s3[8 * y : 8 * y + 8] = r2[pl.ds(y, 8, stride=MSG)]
        s3l[y] = left[y : y + 1]

    @pl.loop(1, wide)
    def _(j):
        q = z_peer(j)
        push(s3.at[rows(q * 8, 8)], n3.at[rows(me_z * 8, 8)], 3, z_id(q))
        push(s3l.at[q], n3l.at[me_z], 4, z_id(q))

    n3[rows(me_z * 8, 8)] = s3[rows(me_z * 8, 8)]
    n3l[me_z] = s3l[me_z]
    drain(n3.at[pl.ds(0, 8 * (wide - 1))], recv.at[3])
    drain(n3l.at[pl.ds(0, wide - 1)], recv.at[4])
    spectral = inverse_z(
        n3[...], n3l[...].reshape(wide, 128), (mix_hi[...], mix_lo[...]), tabs
    )
    drain(fld.at[pl.ds(0, 32 * (wide - 1))], recv.at[1])
    first = second = None
    for x in range(4):
        value = spectral[:, 128 * x : 128 * x + 128] + fld[pl.ds(x, channels, stride=4)]
        summed[x] = value
        first = value if x == 0 else first + value
        second = value * value if x == 0 else second + value * value
    row = stats_row(group_partials(first), group_partials(second))
    st0[0] = row
    ar1[me_z] = row

    @pl.loop(1, wide)
    def _(j):
        push(st0.at[0], ar1.at[me_z], 5, z_id(z_peer(j)))

    drain(ar1.at[pl.ds(0, wide - 1)], recv.at[5])
    row = jnp.sum(ar1[...].reshape(wide, 128), axis=0, keepdims=True)
    st1[0] = row
    ar2[me_x] = row

    @pl.loop(1, narrow)
    def _(j):
        push(st1.at[0], ar2.at[me_x], 6, x_id(x_peer(j)))

    drain(ar2.at[pl.ds(0, narrow - 1)], recv.at[6])
    row = jnp.sum(ar2[...].reshape(narrow, 128), axis=0, keepdims=True)
    mean, inv = stats_columns(row, sizes["count"], channels)
    mean = jnp.broadcast_to(mean, (channels, 128))
    scale = jnp.broadcast_to(inv, (channels, 128)) * cols[0]
    wide_in, wide_out = (in_hi[...], in_lo[...]), (out_hi[...], out_lo[...])
    for x in range(4):
        value = summed[x]
        normed = (value - mean) * scale + cols[1]
        hidden = gelu(dot3(wide_in, split(normed)) + cols[2])
        out[pl.ds(x, channels, stride=4)] = value + dot3(wide_out, split(hidden)) + cols[3]

    drain(b1.at[pl.ds(0, MSG * (narrow - 1))], send.at[0])
    drain(src.at[pl.ds(0, 32 * (wide - 1))], send.at[1])
    drain(b2.at[pl.ds(0, MSG * (narrow - 1))], send.at[2])
    drain(s3.at[pl.ds(0, 8 * (wide - 1))], send.at[3])
    drain(s3l.at[pl.ds(0, wide - 1)], send.at[4])
    drain(ar1.at[pl.ds(0, wide - 1)], send.at[5])
    drain(ar2.at[pl.ds(0, narrow - 1)], send.at[6])


def solution(mesh):
    shape = mesh.shape
    wide, narrow = shape["sp"] * shape["rep"], shape["sub"]
    replicated = P()
    placed = (P(("grp", "sp", "rep"), "sub", None, None),) + (replicated,) * 10

    def local(
        field, mix_weight, factor_x, factor_y, factor_z,
        norm_gain, norm_bias, w_in, b_in, w_out, b_out,
    ):
        held, x_local, ny, nz = field.shape
        channels = mix_weight.shape[0]
        nx = x_local * narrow
        kz = factor_z.shape[1]
        tables = build_tables(nx, ny, nz, kz, held, wide)
        sizes = dict(
            wide=wide, narrow=narrow, channels=channels, rep=shape["rep"],
            count=GROUP_CHANNELS * nx * ny * nz,
        )
        row = lambda v: v.reshape(1, -1)
        operands = [
            field.reshape(held * x_local * ny, nz), factor_x, factor_y, factor_z, mix_weight,
            row(norm_gain), row(norm_bias), w_in, row(b_in), w_out, row(b_out),
        ] + [jnp.asarray(tables[name]) for name in TABLES]
        cells = channels * x_local
        vmem = pl.BlockSpec(memory_space=pltpu.VMEM)
        f32 = lambda *dims: pltpu.VMEM(dims, F32)
        b16 = lambda *dims: pltpu.VMEM(dims, BF16)
        square = (channels, channels)
        result = pl.pallas_call(
            lambda *refs: fused(sizes, *refs),
            out_shape=jax.ShapeDtypeStruct((cells, nz), F32),
            in_specs=[vmem] * len(operands),
            out_specs=vmem,
            scratch_shapes=[
                f32(cells, nz), f32(cells, nz),
                f32(MSG * narrow, 128), f32(MSG * narrow, 128),
                f32(MSG * narrow, 128), f32(MSG * narrow, 128),
                f32(channels, 128), f32(channels, 128),
                f32(wide, 1, 128), f32(wide, 1, 128),
                f32(1, 1, 128), f32(wide, 1, 128), f32(1, 1, 128), f32(narrow, 1, 128),
                f32(ny, 9 * 128),
                b16(*square), b16(*square), b16(*square), b16(*square), b16(*square), b16(*square),
                f32(4, channels, 128), f32(x_local, channels, 128),
                pltpu.SemaphoreType.DMA((7,)), pltpu.SemaphoreType.DMA((7,)),
            ],
            compiler_params=pltpu.CompilerParams(collective_id=0, has_side_effects=True),
        )(*operands)
        return result.reshape(channels, x_local, 1, nz)

    return jax.shard_map(
        local,
        mesh=mesh,
        in_specs=placed,
        out_specs=P("grp", "sub", ("sp", "rep"), None),
        check_vma=False,
    )
```

```python
import functools
import math

import jax
import jax.numpy as jnp
import numpy as np
from jax import lax
from jax.experimental import pallas as pl
from jax.experimental.pallas import tpu as pltpu
from jax.sharding import PartitionSpec as P

F32 = jnp.float32
BF16 = jnp.bfloat16
GROUP_CHANNELS = 8
EPS = 1e-05


def split_np(a):
    a = np.asarray(a, np.float32)
    hi = a.astype(BF16)
    lo = (a - hi.astype(np.float32)).astype(BF16)
    return hi, lo


def build_tables(nx, ny, nz, kz, ch_local, wide):
    xl = 4
    chunks = 8
    lane = np.arange(128)
    k_of, x_of, r_of = lane // 16, (lane // 4) % 4, lane % 4
    z = np.arange(nz)
    scale = 1.0 / (nx * ny * nz)
    top = kz // 2
    fwd_z = np.zeros((xl, nz, 256))
    inv_z = np.zeros((256, xl, nz))
    for l in range(128):
        f = 2 * k_of[l] + r_of[l] // 2
        ang = 2 * np.pi * ((f * z) % nz) / nz
        fwd_z[x_of[l], :, l] = (np.cos(ang) if r_of[l] % 2 == 0 else -np.sin(ang)) * scale
        inv_z[l, x_of[l], :] = np.cos(ang) if r_of[l] % 2 == 0 else -np.sin(ang)
        if r_of[l] < 2:
            ang = 2 * np.pi * ((top * z) % nz) / nz
            col = np.cos(ang) if r_of[l] == 0 else -np.sin(ang)
            fwd_z[x_of[l], :, 128 + l] = col * scale
            inv_z[128 + l, x_of[l], :] = col
    fwd_z = fwd_z.reshape(xl * nz, 256)
    inv_z = inv_z.reshape(256, xl * nz)
    ax = np.arange(nx)
    ang = 2 * np.pi * ((ax[:, None] * ax[None, :]) % nx) / nx
    c, s = np.cos(ang), np.sin(ang)
    fwd = np.zeros((nx, 2, 2, nx, 2, 2))
    inv = np.zeros((nx, 2, 2, nx, 2, 2))
    for f in range(2):
        fwd[:, f, 0, :, f, 0] = c
        fwd[:, f, 1, :, f, 0] = s
        fwd[:, f, 0, :, f, 1] = -s
        fwd[:, f, 1, :, f, 1] = c
        inv[:, f, 0, :, f, 0] = c
        inv[:, f, 1, :, f, 0] = -s
        inv[:, f, 0, :, f, 1] = s
        inv[:, f, 1, :, f, 1] = c
    turn = np.zeros((128, 128))
    for l in range(0, 128, 2):
        turn[l + 1, l] = 1.0
        turn[l, l + 1] = -1.0
    fwd = fwd.reshape(128, 128)
    inv = inv.reshape(128, 128)
    x_fwd = np.concatenate([fwd, fwd @ turn], 1)
    x_inv = np.concatenate([inv, -(inv @ turn)], 1)
    ay = np.arange(ny)
    ang = 2 * np.pi * ((ay[:, None] * ay[None, :]) % ny) / ny
    y_tab = np.concatenate([np.cos(ang), np.sin(ang)], 1)
    hi, lo = split_np(y_tab)
    y_tab3 = np.concatenate([hi, hi, lo], 1)
    sel_x = np.zeros((nx, 256))
    for a in range(nx):
        sel_x[a, 4 * a : 4 * a + 4] = 1.0
        sel_x[a, 128 + 4 * ((nx - a) % nx) : 128 + 4 * ((nx - a) % nx) + 4] = 1.0
    sel_z = np.zeros((kz, 2, 9, nx, 4))
    for f in range(top + 1):
        k, f2 = f // 2, f % 2
        if f < top:
            sel_z[f, 0, k, :, 2 * f2 : 2 * f2 + 2] = 1.0
        if f > 0:
            sel_z[kz - f, 1, k, :, 2 * f2 : 2 * f2 + 2] = 1.0
    sel_z = sel_z.reshape(kz, 2 * 9 * 128)
    rows_in = np.arange(ch_local * ny)
    rows_out = np.arange(ch_local * 8)
    gather = (
        (rows_in[None, :] // ny == rows_out[:, None] // 8)
        & (rows_in[None, :] % 8 == rows_out[:, None] % 8)
    ).astype(np.float32)
    rows_all = np.arange(ch_local * wide)
    spread = (rows_all[:, None] // ch_local == np.arange(wide)[None, :]).astype(np.float32)
    fz = split_np(fwd_z)
    iz = split_np(inv_z)
    xf = split_np(x_fwd)
    xi = split_np(x_inv)
    return dict(
        fz_hi=fz[0], fz_lo=fz[1], iz_hi=iz[0], iz_lo=iz[1],
        xf_hi=xf[0], xf_lo=xf[1], xi_hi=xi[0], xi_lo=xi[1],
        y_tab=y_tab3,
        sel_x=sel_x.astype(np.float32), sel_z=sel_z.astype(np.float32),
        gather=gather.astype(BF16), spread=spread.astype(BF16),
    )


def split(a):
    hi = a.astype(BF16)
    return hi, (a - hi.astype(F32)).astype(BF16)


def dot1(a, b):
    return lax.dot_general(a, b, (((1,), (0,)), ((), ())), preferred_element_type=F32)


def dot3(a, b):
    return dot1(a[0], b[0]) + dot1(a[0], b[1]) + dot1(a[1], b[0])


def swap_chunks(arrays, roll):
    arrays = list(arrays)
    rows = arrays[0].shape[0]
    chunk = lax.broadcasted_iota(jnp.int32, (rows, 128), 1) // 16
    for d in (4, 2, 1):
        upper = (chunk // d) % 2 == 1
        for i in range(8):
            if (i // d) % 2 == 0:
                low, high = arrays[i], arrays[i + d]
                arrays[i] = jnp.where(upper, roll(high, 16 * d), low)
                arrays[i + d] = jnp.where(upper, high, roll(low, 128 - 16 * d))
    return arrays


def forward_z(parts, tabs):
    fz_hi, fz_lo = tabs["fz_hi"], tabs["fz_lo"]
    total = None
    for x, part in enumerate(parts):
        term = dot3(split(part), (fz_hi[128 * x : 128 * x + 128], fz_lo[128 * x : 128 * x + 128]))
        total = term if total is None else total + term
    main, extra = total[:, :128], total[:, 128:]
    rows, lanes = (lax.broadcasted_iota(jnp.int32, extra.shape, d) for d in (0, 1))
    extra = jnp.where((rows % 32) // 8 == lanes // 16, extra, 0.0)
    hi, lo = split(extra)
    packed = dot1(tabs["gather"], hi) + dot1(tabs["gather"], lo)
    return main, packed


def factor_weights(fac_x, fac_y, fac_z, channel, tabs):
    n, channels = fac_y.shape
    own = lax.broadcasted_iota(jnp.int32, (n, channels), 1) == channel
    col_x, col_y, col_z = (
        jnp.sum(jnp.where(own, f, 0.0), axis=1, keepdims=True) for f in (fac_x, fac_y, fac_z)
    )
    lanes_x = jnp.sum(col_x * tabs["sel_x"], axis=0, keepdims=True)
    lanes_z = jnp.sum(col_z * tabs["sel_z"], axis=0, keepdims=True)
    plus = lanes_z[:, :1152] * jnp.concatenate([lanes_x[:, :128]] * 9, 1)
    minus = lanes_z[:, 1152:] * jnp.concatenate([lanes_x[:, 128:]] * 9, 1)
    r, c = (lax.broadcasted_iota(jnp.int32, (n, n), d) for d in (0, 1))
    row_y = jnp.sum(jnp.where(r == c, col_y, 0.0), axis=0, keepdims=True)
    flipped = jnp.where((n - r) % n == c, jnp.broadcast_to(row_y, (n, n)), 0.0)
    col_minus = jnp.sum(flipped, axis=1, keepdims=True)
    return col_y * plus + col_minus * minus


def spectral_filter(blocks, weights, tabs, roll):
    main = swap_chunks([b[:32] for b in blocks], roll)
    extra = swap_chunks([b[32:40] for b in blocks], roll)
    last = jnp.concatenate(extra[:4], 0)
    rows = jnp.concatenate(main + [last], 0)

    def along_y(pairs):
        stacked = jnp.concatenate(
            [
                jnp.concatenate(
                    [pairs[32 * k : 32 * k + 32, :128], pairs[32 * k : 32 * k + 32, 128:]], 0
                )
                for k in range(9)
            ],
            1,
        )
        hi, lo = split(stacked)
        return dot1(tabs["y_tab"], jnp.concatenate([hi, lo, hi], 0))

    pairs = dot3(split(rows), (tabs["xf_hi"], tabs["xf_lo"]))
    spec = along_y(pairs) * weights
    rows = jnp.concatenate([spec[:, 128 * k : 128 * k + 128] for k in range(9)], 0)
    pairs = dot3(split(rows), (tabs["xi_hi"], tabs["xi_lo"]))
    back = along_y(pairs)
    main = swap_chunks([back[:, 128 * k : 128 * k + 128] for k in range(8)], roll)
    last = back[:, 1024:]
    tiles = [last[8 * p : 8 * p + 8] for p in range(4)] + [jnp.zeros((8, 128), F32)] * 4
    extra = swap_chunks(tiles, roll)
    return main, extra


def leftover_rows(extras, roll):
    return jnp.concatenate(swap_chunks(extras, roll)[:4], 0)


def inverse_z(modes, left, mix, tabs):
    hi, lo = split(left)
    wide = dot1(tabs["spread"], hi) + dot1(tabs["spread"], lo)
    rows, lanes = (lax.broadcasted_iota(jnp.int32, wide.shape, d) for d in (0, 1))
    wide = jnp.where(rows % 8 == lanes // 16, wide, 0.0)
    both = jnp.concatenate([modes, wide], 1)
    mixed = dot3(mix, split(both))
    return dot3(split(mixed), (tabs["iz_hi"], tabs["iz_lo"]))


def to_column(row):
    n = row.shape[1]
    r, c = (lax.broadcasted_iota(jnp.int32, (n, n), d) for d in (0, 1))
    return jnp.sum(jnp.where(r == c, jnp.broadcast_to(row, (n, n)), 0.0), axis=1, keepdims=True)


def group_partials(total):
    folded = jnp.sum(total.reshape(total.shape[0] // 8, 8, 128), axis=1)
    return jnp.sum(folded, axis=1, keepdims=True)


def stats_row(first, second):
    n = first.shape[0]
    r, c = (lax.broadcasted_iota(jnp.int32, (n, 128), d) for d in (0, 1))
    placed = jnp.where(r == c, first, 0.0) + jnp.where(r + n == c, second, 0.0)
    return jnp.sum(placed, axis=0, keepdims=True)


def stats_columns(row, count, channels):
    groups = channels // GROUP_CHANNELS
    r, c = (lax.broadcasted_iota(jnp.int32, (channels, 128), d) for d in (0, 1))
    wide = jnp.broadcast_to(row, (channels, 128))
    first = jnp.sum(jnp.where(r // GROUP_CHANNELS == c, wide, 0.0), axis=1, keepdims=True)
    second = jnp.sum(
        jnp.where(r // GROUP_CHANNELS + groups == c, wide, 0.0), axis=1, keepdims=True
    )
    mean = first / count
    var = second / count - mean * mean
    return mean, lax.rsqrt(var + EPS)


def gelu(v):
    inner = math.sqrt(2.0 / math.pi) * (v + 0.044715 * (v * v * v))
    return 0.5 * v * (1.0 + jnp.tanh(inner))


TABLES = (
    "fz_hi", "fz_lo", "iz_hi", "iz_lo", "xf_hi", "xf_lo", "xi_hi", "xi_lo",
    "y_tab", "sel_x", "sel_z", "gather", "spread",
)
MSG = 40


class Lazy:
    def __init__(self, refs):
        self.refs = refs

    def __getitem__(self, name):
        return self.refs[name][...]


def lane_roll(a, shift):
    return pltpu.roll(a, shift, axis=1)


def fused(sizes, *refs):
    wide, narrow, channels = sizes["wide"], sizes["narrow"], sizes["channels"]
    rep = sizes["rep"]
    count = 5 + len(TABLES)
    given, out = refs[:count], refs[count : count + 2]
    scratch = refs[count + 2 :]
    held, loaded, scratch = scratch[:count], scratch[count], scratch[count + 1 :]
    (field, fac_x, fac_y, fac_z, mix) = held[:5]
    tabs = Lazy(dict(zip(TABLES, held[5:])))
    where_is = {name: 5 + n for n, name in enumerate(TABLES)}
    (
        src, fld, b1, r1, b2, r2, s3, n3, s3l, n3l, st0, ar1, st1, ar2,
        wts, mix_hi, mix_lo, send, recv, ready,
    ) = scratch
    me_x, me_sp, me_rep = lax.axis_index("sub"), lax.axis_index("sp"), lax.axis_index("rep")
    me_z = me_sp * rep + me_rep
    channel = me_z * narrow + me_x
    chips = wide // rep
    turn = jnp.where(me_sp == 0, chips - 1, me_sp - 1)

    def chip_at(position):
        return jnp.where(position == chips - 1, 0, position + 1)

    def z_id(sp, core):
        return {"sp": sp, "rep": core}

    def x_id(s):
        return {"sub": s}

    def x_peer(j):
        s = me_x + j
        return jnp.where(s >= narrow, s - narrow, s)

    def signal(sem, where):
        pl.semaphore_signal(sem, inc=1, device_id=where, device_id_type=pl.DeviceIdType.MESH)

    def push(a, b, slot, where):
        pltpu.make_async_remote_copy(
            src_ref=a, dst_ref=b, send_sem=send.at[slot], recv_sem=recv.at[slot],
            device_id=where, device_id_type=pl.DeviceIdType.MESH,
        ).start()

    def drain(ref, sem):
        pltpu.make_async_copy(ref, ref, sem).wait()

    def rows(start, size):
        return pl.ds(pl.multiple_of(start, 8), size)

    barrier = pltpu.get_barrier_semaphore()

    @pl.loop(1, narrow)
    def _(j):
        signal(barrier, x_id(x_peer(j)))

    for core in range(1, rep):
        signal(barrier, {"rep": (me_rep + core) % rep})

    loads = [
        pltpu.make_async_copy(a, b, loaded.at[n]) for n, (a, b) in enumerate(zip(given, held))
    ]
    first = [0, where_is["fz_hi"], where_is["fz_lo"], where_is["gather"]]
    later = [n for n in range(count) if n not in first]
    for n in first + later:
        loads[n].start()
    for n in first:
        loads[n].wait()
    parts = [
        jnp.concatenate([field[128 * c + 32 * x : 128 * c + 32 * x + 32] for c in range(8)], 0)
        for x in range(4)
    ]
    main, packed = forward_z(parts, tabs)
    for c in range(8):
        b1[MSG * c : MSG * c + 32] = main[32 * c : 32 * c + 32]
        b1[MSG * c + 32 : MSG * c + 40] = packed[8 * c : 8 * c + 8]
    for y in range(32):
        src[32 * y : 32 * y + 32] = field[pl.ds(y, 32, stride=32)]

    pl.semaphore_wait(barrier, narrow - 1 + rep - 1 + rep * jnp.minimum(turn, 1))

    @pl.when(turn < chips - 1)
    def _():
        for core in range(rep):
            signal(barrier, z_id(chip_at(turn + 1), core))

    @pl.loop(1, narrow)
    def _(j):
        s = x_peer(j)
        push(b1.at[rows(s * MSG, MSG)], r1.at[rows(me_x * MSG, MSG)], 0, x_id(s))

    @pl.loop(0, turn)
    def _(position):
        for core in range(rep):
            signal(ready.at[me_z], z_id(chip_at(position), core))

    def send_field(sp, core):
        q = sp * rep + core
        push(src.at[rows(q * 32, 32)], fld.at[rows(me_z * 32, 32)], 1, z_id(sp, core))

    def send_modes(sp, core):
        q = sp * rep + core
        push(s3.at[rows(q * 8, 8)], n3.at[rows(me_z * 8, 8)], 3, z_id(sp, core))
        push(s3l.at[q], n3l.at[me_z], 4, z_id(sp, core))

    @pl.loop(0, turn)
    def _(position):
        for core in range(rep):
            send_field(chip_at(position), core)

    for core in range(1, rep):
        send_field(me_sp, (me_rep + core) % rep)

    r1[rows(me_x * MSG, MSG)] = b1[rows(me_x * MSG, MSG)]
    fld[rows(me_z * 32, 32)] = src[rows(me_z * 32, 32)]
    for n in later:
        loads[n].wait()
    wts[...] = factor_weights(fac_x[...], fac_y[...], fac_z[...], channel, tabs)
    mix_hi[...], mix_lo[...] = split(mix[...])

    drain(r1.at[pl.ds(0, MSG * (narrow - 1))], recv.at[0])
    blocks = [r1[MSG * s : MSG * s + MSG] for s in range(8)]
    main, extra = spectral_filter(blocks, wts[...], tabs, lane_roll)
    for s in range(8):
        b2[MSG * s : MSG * s + 32] = main[s]
        b2[MSG * s + 32 : MSG * s + 40] = extra[s]

    @pl.loop(1, narrow)
    def _(j):
        s = x_peer(j)
        push(b2.at[rows(s * MSG, MSG)], r2.at[rows(me_x * MSG, MSG)], 2, x_id(s))

    r2[rows(me_x * MSG, MSG)] = b2[rows(me_x * MSG, MSG)]
    drain(r2.at[pl.ds(0, MSG * (narrow - 1))], recv.at[2])
    left = leftover_rows([r2[MSG * c + 32 : MSG * c + 40] for c in range(8)], lane_roll)
    for y in range(32):
        s3[8 * y : 8 * y + 8] = r2[pl.ds(y, 8, stride=MSG)]
        s3l[y] = left[y : y + 1]

    @pl.loop(0, turn)
    def _(position):
        for core in range(rep):
            send_modes(chip_at(position), core)

    for core in range(1, rep):
        send_modes(me_sp, (me_rep + core) % rep)

    @pl.loop(turn + 1, chips)
    def _(position):
        sp = chip_at(position)
        for core in range(rep):
            pl.semaphore_wait(ready.at[sp * rep + core], 1)
            send_modes(sp, core)
            send_field(sp, core)

    n3[rows(me_z * 8, 8)] = s3[rows(me_z * 8, 8)]
    n3l[me_z] = s3l[me_z]
    drain(n3.at[pl.ds(0, 8 * (wide - 1))], recv.at[3])
    drain(n3l.at[pl.ds(0, wide - 1)], recv.at[4])
    spectral = inverse_z(
        n3[...], n3l[...].reshape(wide, 128), (mix_hi[...], mix_lo[...]), tabs
    )
    drain(fld.at[pl.ds(0, 32 * (wide - 1))], recv.at[1])
    first = second = None
    for x in range(4):
        value = spectral[:, 128 * x : 128 * x + 128] + fld[pl.ds(x, channels, stride=4)]
        out[0][x] = value
        first = value if x == 0 else first + value
        second = value * value if x == 0 else second + value * value
    row = stats_row(group_partials(first), group_partials(second))
    st0[0] = row
    ar1[me_z] = row

    for step in sorted(range(1, chips), key=lambda d: -min(d, chips - d)):
        sp = me_sp + step
        sp = jnp.where(sp >= chips, sp - chips, sp)
        for core in range(rep):
            push(st0.at[0], ar1.at[me_z], 5, z_id(sp, core))
    for core in range(1, rep):
        push(st0.at[0], ar1.at[me_z], 5, z_id(me_sp, (me_rep + core) % rep))

    drain(ar1.at[pl.ds(0, wide - 1)], recv.at[5])
    row = jnp.sum(ar1[...].reshape(wide, 128), axis=0, keepdims=True)
    st1[0] = row
    ar2[me_x] = row

    @pl.loop(1, narrow)
    def _(j):
        push(st1.at[0], ar2.at[me_x], 6, x_id(x_peer(j)))

    drain(ar2.at[pl.ds(0, narrow - 1)], recv.at[6])
    row = jnp.sum(ar2[...].reshape(narrow, 128), axis=0, keepdims=True)
    out[1][...] = row

    drain(b1.at[pl.ds(0, MSG * (narrow - 1))], send.at[0])
    drain(src.at[pl.ds(0, 32 * (wide - 1))], send.at[1])
    drain(b2.at[pl.ds(0, MSG * (narrow - 1))], send.at[2])
    drain(s3.at[pl.ds(0, 8 * (wide - 1))], send.at[3])
    drain(s3l.at[pl.ds(0, wide - 1)], send.at[4])
    drain(ar1.at[pl.ds(0, wide - 1)], send.at[5])
    drain(ar2.at[pl.ds(0, narrow - 1)], send.at[6])


def channel_mlp(count, summed, stats, gain, bias, w_in, b_in, w_out, b_out, out):
    channels = summed.shape[1]
    mean, inv = stats_columns(stats[...], count, channels)
    scale = inv * to_column(gain[...])
    shift, col_in, col_out = (to_column(v[...]) for v in (bias, b_in, b_out))
    wide_in, wide_out = split(w_in[...]), split(w_out[...])
    for x in range(summed.shape[0]):
        value = summed[x]
        normed = (value - mean) * scale + shift
        hidden = gelu(dot3(wide_in, split(normed)) + col_in)
        out[pl.ds(x, channels, stride=4)] = value + dot3(wide_out, split(hidden)) + col_out


def solution(mesh):
    shape = mesh.shape
    wide, narrow = shape["sp"] * shape["rep"], shape["sub"]
    replicated = P()
    placed = (P(("grp", "sp", "rep"), "sub", None, None),) + (replicated,) * 10

    def local(
        field, mix_weight, factor_x, factor_y, factor_z,
        norm_gain, norm_bias, w_in, b_in, w_out, b_out,
    ):
        held, x_local, ny, nz = field.shape
        channels = mix_weight.shape[0]
        nx = x_local * narrow
        kz = factor_z.shape[1]
        tables = build_tables(nx, ny, nz, kz, held, wide)
        sizes = dict(
            wide=wide, narrow=narrow, channels=channels, rep=shape["rep"],
            count=GROUP_CHANNELS * nx * ny * nz,
        )
        row = lambda v: v.reshape(1, -1)
        operands = [
            field.reshape(held * x_local * ny, nz), factor_x.T, factor_y.T, factor_z.T, mix_weight,
        ] + [jnp.asarray(tables[name]) for name in TABLES]
        cells = channels * x_local
        vmem = pl.BlockSpec(memory_space=pltpu.VMEM)
        f32 = lambda *dims: pltpu.VMEM(dims, F32)
        b16 = lambda *dims: pltpu.VMEM(dims, BF16)
        square = (channels, channels)
        summed, stats = pl.pallas_call(
            lambda *refs: fused(sizes, *refs),
            out_shape=(
                jax.ShapeDtypeStruct((x_local, channels, nz), F32),
                jax.ShapeDtypeStruct((1, 128), F32),
            ),
            in_specs=[pl.BlockSpec(memory_space=pl.ANY)] * len(operands),
            out_specs=(vmem, vmem),
            scratch_shapes=[pltpu.VMEM(v.shape, v.dtype) for v in operands]
            + [pltpu.SemaphoreType.DMA((len(operands),))]
            + [
                f32(cells, nz), f32(cells, nz),
                f32(MSG * narrow, 128), f32(MSG * narrow, 128),
                f32(MSG * narrow, 128), f32(MSG * narrow, 128),
                f32(channels, 128), f32(channels, 128),
                f32(wide, 1, 128), f32(wide, 1, 128),
                f32(1, 1, 128), f32(wide, 1, 128), f32(1, 1, 128), f32(narrow, 1, 128),
                f32(ny, 9 * 128),
                b16(*square), b16(*square),
                pltpu.SemaphoreType.DMA((7,)), pltpu.SemaphoreType.DMA((7,)),
                pltpu.SemaphoreType.REGULAR((wide,)),
            ],
            compiler_params=pltpu.CompilerParams(collective_id=0, has_side_effects=True),
        )(*operands)
        result = pl.pallas_call(
            functools.partial(channel_mlp, sizes["count"]),
            out_shape=jax.ShapeDtypeStruct((cells, nz), F32),
            in_specs=[vmem] * 8,
            out_specs=vmem,
        )(summed, stats, row(norm_gain), row(norm_bias), w_in, row(b_in), w_out, row(b_out))
        return result.reshape(channels, x_local, 1, nz)

    return jax.shard_map(
        local,
        mesh=mesh,
        in_specs=placed,
        out_specs=P("grp", "sub", ("sp", "rep"), None),
        check_vma=False,
    )
```

```python
import functools
import math

import jax
import jax.numpy as jnp
import numpy as np
from jax import lax
from jax.experimental import pallas as pl
from jax.experimental.pallas import tpu as pltpu
from jax.sharding import PartitionSpec as P

F32 = jnp.float32
BF16 = jnp.bfloat16
GROUP_CHANNELS = 8
EPS = 1e-05


def split_np(a):
    a = np.asarray(a, np.float32)
    hi = a.astype(BF16)
    lo = (a - hi.astype(np.float32)).astype(BF16)
    return hi, lo


def build_tables(nx, ny, nz, kz, ch_local, wide):
    xl = 4
    chunks = 8
    lane = np.arange(128)
    k_of, x_of, r_of = lane // 16, (lane // 4) % 4, lane % 4
    z = np.arange(nz)
    scale = 1.0 / (nx * ny * nz)
    top = kz // 2
    fwd_z = np.zeros((xl, nz, 256))
    inv_z = np.zeros((256, xl, nz))
    for l in range(128):
        f = 2 * k_of[l] + r_of[l] // 2
        ang = 2 * np.pi * ((f * z) % nz) / nz
        fwd_z[x_of[l], :, l] = (np.cos(ang) if r_of[l] % 2 == 0 else -np.sin(ang)) * scale
        inv_z[l, x_of[l], :] = np.cos(ang) if r_of[l] % 2 == 0 else -np.sin(ang)
        if r_of[l] < 2:
            ang = 2 * np.pi * ((top * z) % nz) / nz
            col = np.cos(ang) if r_of[l] == 0 else -np.sin(ang)
            fwd_z[x_of[l], :, 128 + l] = col * scale
            inv_z[128 + l, x_of[l], :] = col
    fwd_z = fwd_z.reshape(xl * nz, 256)
    inv_z = inv_z.reshape(256, xl * nz)
    ax = np.arange(nx)
    ang = 2 * np.pi * ((ax[:, None] * ax[None, :]) % nx) / nx
    c, s = np.cos(ang), np.sin(ang)
    fwd = np.zeros((nx, 2, 2, nx, 2, 2))
    inv = np.zeros((nx, 2, 2, nx, 2, 2))
    for f in range(2):
        fwd[:, f, 0, :, f, 0] = c
        fwd[:, f, 1, :, f, 0] = s
        fwd[:, f, 0, :, f, 1] = -s
        fwd[:, f, 1, :, f, 1] = c
        inv[:, f, 0, :, f, 0] = c
        inv[:, f, 1, :, f, 0] = -s
        inv[:, f, 0, :, f, 1] = s
        inv[:, f, 1, :, f, 1] = c
    turn = np.zeros((128, 128))
    for l in range(0, 128, 2):
        turn[l + 1, l] = 1.0
        turn[l, l + 1] = -1.0
    fwd = fwd.reshape(128, 128)
    inv = inv.reshape(128, 128)
    x_fwd = np.concatenate([fwd, fwd @ turn], 1)
    x_inv = np.concatenate([inv, -(inv @ turn)], 1)
    ay = np.arange(ny)
    ang = 2 * np.pi * ((ay[:, None] * ay[None, :]) % ny) / ny
    y_tab = np.concatenate([np.cos(ang), np.sin(ang)], 1)
    hi, lo = split_np(y_tab)
    y_tab3 = np.concatenate([hi, hi, lo], 1)
    sel_x = np.zeros((nx, 256))
    for a in range(nx):
        sel_x[a, 4 * a : 4 * a + 4] = 1.0
        sel_x[a, 128 + 4 * ((nx - a) % nx) : 128 + 4 * ((nx - a) % nx) + 4] = 1.0
    sel_z = np.zeros((kz, 2, 9, nx, 4))
    for f in range(top + 1):
        k, f2 = f // 2, f % 2
        if f < top:
            sel_z[f, 0, k, :, 2 * f2 : 2 * f2 + 2] = 1.0
        if f > 0:
            sel_z[kz - f, 1, k, :, 2 * f2 : 2 * f2 + 2] = 1.0
    sel_z = sel_z.reshape(kz, 2 * 9 * 128)
    rows_in = np.arange(ch_local * ny)
    rows_out = np.arange(ch_local * 8)
    gather = (
        (rows_in[None, :] // ny == rows_out[:, None] // 8)
        & (rows_in[None, :] % 8 == rows_out[:, None] % 8)
    ).astype(np.float32)
    rows_all = np.arange(ch_local * wide)
    spread = (rows_all[:, None] // ch_local == np.arange(wide)[None, :]).astype(np.float32)
    fz = split_np(fwd_z)
    iz = split_np(inv_z)
    xf = split_np(x_fwd)
    xi = split_np(x_inv)
    return dict(
        fz_hi=fz[0], fz_lo=fz[1], iz_hi=iz[0], iz_lo=iz[1],
        xf_hi=xf[0], xf_lo=xf[1], xi_hi=xi[0], xi_lo=xi[1],
        y_tab=y_tab3,
        sel_x=sel_x.astype(np.float32), sel_z=sel_z.astype(np.float32),
        gather=gather.astype(BF16), spread=spread.astype(BF16),
    )


def split(a):
    hi = a.astype(BF16)
    return hi, (a - hi.astype(F32)).astype(BF16)


def dot1(a, b):
    return lax.dot_general(a, b, (((1,), (0,)), ((), ())), preferred_element_type=F32)


def dot3(a, b):
    return dot1(a[0], b[0]) + dot1(a[0], b[1]) + dot1(a[1], b[0])


def swap_chunks(arrays, roll):
    arrays = list(arrays)
    rows = arrays[0].shape[0]
    chunk = lax.broadcasted_iota(jnp.int32, (rows, 128), 1) // 16
    for d in (4, 2, 1):
        upper = (chunk // d) % 2 == 1
        for i in range(8):
            if (i // d) % 2 == 0:
                low, high = arrays[i], arrays[i + d]
                arrays[i] = jnp.where(upper, roll(high, 16 * d), low)
                arrays[i + d] = jnp.where(upper, high, roll(low, 128 - 16 * d))
    return arrays


def forward_z(parts, tabs):
    fz_hi, fz_lo = tabs["fz_hi"], tabs["fz_lo"]
    total = None
    for x, part in enumerate(parts):
        term = dot3(split(part), (fz_hi[128 * x : 128 * x + 128], fz_lo[128 * x : 128 * x + 128]))
        total = term if total is None else total + term
    main, extra = total[:, :128], total[:, 128:]
    rows, lanes = (lax.broadcasted_iota(jnp.int32, extra.shape, d) for d in (0, 1))
    extra = jnp.where((rows % 32) // 8 == lanes // 16, extra, 0.0)
    hi, lo = split(extra)
    packed = dot1(tabs["gather"], hi) + dot1(tabs["gather"], lo)
    return main, packed


def factor_weights(fac_x, fac_y, fac_z, channel, tabs):
    n, channels = fac_y.shape
    own = lax.broadcasted_iota(jnp.int32, (n, channels), 1) == channel
    col_x, col_y, col_z = (
        jnp.sum(jnp.where(own, f, 0.0), axis=1, keepdims=True) for f in (fac_x, fac_y, fac_z)
    )
    lanes_x = jnp.sum(col_x * tabs["sel_x"], axis=0, keepdims=True)
    lanes_z = jnp.sum(col_z * tabs["sel_z"], axis=0, keepdims=True)
    plus = lanes_z[:, :1152] * jnp.concatenate([lanes_x[:, :128]] * 9, 1)
    minus = lanes_z[:, 1152:] * jnp.concatenate([lanes_x[:, 128:]] * 9, 1)
    r, c = (lax.broadcasted_iota(jnp.int32, (n, n), d) for d in (0, 1))
    row_y = jnp.sum(jnp.where(r == c, col_y, 0.0), axis=0, keepdims=True)
    flipped = jnp.where((n - r) % n == c, jnp.broadcast_to(row_y, (n, n)), 0.0)
    col_minus = jnp.sum(flipped, axis=1, keepdims=True)
    return col_y * plus + col_minus * minus


def spectral_filter(blocks, weights, tabs, roll):
    main = swap_chunks([b[:32] for b in blocks], roll)
    extra = swap_chunks([b[32:40] for b in blocks], roll)
    last = jnp.concatenate(extra[:4], 0)
    rows = jnp.concatenate(main + [last], 0)

    def along_y(pairs):
        stacked = jnp.concatenate(
            [
                jnp.concatenate(
                    [pairs[32 * k : 32 * k + 32, :128], pairs[32 * k : 32 * k + 32, 128:]], 0
                )
                for k in range(9)
            ],
            1,
        )
        hi, lo = split(stacked)
        return dot1(tabs["y_tab"], jnp.concatenate([hi, lo, hi], 0))

    pairs = dot3(split(rows), (tabs["xf_hi"], tabs["xf_lo"]))
    spec = along_y(pairs) * weights
    rows = jnp.concatenate([spec[:, 128 * k : 128 * k + 128] for k in range(9)], 0)
    pairs = dot3(split(rows), (tabs["xi_hi"], tabs["xi_lo"]))
    back = along_y(pairs)
    main = swap_chunks([back[:, 128 * k : 128 * k + 128] for k in range(8)], roll)
    last = back[:, 1024:]
    tiles = [last[8 * p : 8 * p + 8] for p in range(4)] + [jnp.zeros((8, 128), F32)] * 4
    extra = swap_chunks(tiles, roll)
    return main, extra


def leftover_rows(extras, roll):
    return jnp.concatenate(swap_chunks(extras, roll)[:4], 0)


def inverse_z(modes, left, mix, tabs):
    hi, lo = split(left)
    wide = dot1(tabs["spread"], hi) + dot1(tabs["spread"], lo)
    rows, lanes = (lax.broadcasted_iota(jnp.int32, wide.shape, d) for d in (0, 1))
    wide = jnp.where(rows % 8 == lanes // 16, wide, 0.0)
    both = jnp.concatenate([modes, wide], 1)
    mixed = dot3(mix, split(both))
    return dot3(split(mixed), (tabs["iz_hi"], tabs["iz_lo"]))


def to_column(row):
    n = row.shape[1]
    r, c = (lax.broadcasted_iota(jnp.int32, (n, n), d) for d in (0, 1))
    return jnp.sum(jnp.where(r == c, jnp.broadcast_to(row, (n, n)), 0.0), axis=1, keepdims=True)


def group_partials(total):
    folded = jnp.sum(total.reshape(total.shape[0] // 8, 8, 128), axis=1)
    return jnp.sum(folded, axis=1, keepdims=True)


def stats_row(first, second):
    n = first.shape[0]
    r, c = (lax.broadcasted_iota(jnp.int32, (n, 128), d) for d in (0, 1))
    placed = jnp.where(r == c, first, 0.0) + jnp.where(r + n == c, second, 0.0)
    return jnp.sum(placed, axis=0, keepdims=True)


def stats_columns(row, count, channels):
    groups = channels // GROUP_CHANNELS
    r, c = (lax.broadcasted_iota(jnp.int32, (channels, 128), d) for d in (0, 1))
    wide = jnp.broadcast_to(row, (channels, 128))
    first = jnp.sum(jnp.where(r // GROUP_CHANNELS == c, wide, 0.0), axis=1, keepdims=True)
    second = jnp.sum(
        jnp.where(r // GROUP_CHANNELS + groups == c, wide, 0.0), axis=1, keepdims=True
    )
    mean = first / count
    var = second / count - mean * mean
    return mean, lax.rsqrt(var + EPS)


def gelu(v):
    inner = math.sqrt(2.0 / math.pi) * (v + 0.044715 * (v * v * v))
    return 0.5 * v * (1.0 + jnp.tanh(inner))


TABLES = (
    "fz_hi", "fz_lo", "iz_hi", "iz_lo", "xf_hi", "xf_lo", "xi_hi", "xi_lo",
    "y_tab", "sel_x", "sel_z", "gather", "spread",
)
MSG = 40


class Lazy:
    def __init__(self, refs):
        self.refs = refs

    def __getitem__(self, name):
        return self.refs[name][...]


def lane_roll(a, shift):
    return pltpu.roll(a, shift, axis=1)


def far_first(n):
    return sorted(range(1, n), key=lambda d: -min(d, n - d))


AHEAD = 4


def fused(sizes, *refs):
    wide, narrow, channels = sizes["wide"], sizes["narrow"], sizes["channels"]
    rep = sizes["rep"]
    count = 5 + len(TABLES)
    given, out = refs[:count], refs[count : count + 2]
    scratch = refs[count + 2 :]
    held, loaded, scratch = scratch[:count], scratch[count], scratch[count + 1 :]
    (field, fac_x, fac_y, fac_z, mix) = held[:5]
    tabs = Lazy(dict(zip(TABLES, held[5:])))
    where_is = {name: 5 + n for n, name in enumerate(TABLES)}
    (
        src, fld, b1, r1, b2, r2, s3, n3, st0, ar1, st1, ar2,
        wts, mix_hi, mix_lo, send, recv, ready,
    ) = scratch
    me_x, me_sp, me_rep = lax.axis_index("sub"), lax.axis_index("sp"), lax.axis_index("rep")
    me_z = me_sp * rep + me_rep
    channel = me_z * narrow + me_x
    chips = wide // rep
    last = (me_sp == 0) & (me_rep == 0)
    turn = jnp.where(last, chips, me_sp)

    def each(low, high, action):
        @pl.loop(low, high)
        def _(position):
            sp = jnp.where(position == chips, 0, position)
            for core in range(rep):

                @pl.when(position > 0 if core == 0 else position < chips)
                def _():
                    action(sp, core)

    def partners(action):
        @pl.when(me_sp > 0)
        def _():
            for core in range(1, rep):
                action(me_sp, (me_rep + core) % rep)

    def z_id(sp, core):
        return {"sp": sp, "rep": core}

    def x_id(s):
        return {"sub": s}

    def x_peer(j):
        s = me_x + j
        return jnp.where(s >= narrow, s - narrow, s)

    def signal(sem, where):
        pl.semaphore_signal(sem, inc=1, device_id=where, device_id_type=pl.DeviceIdType.MESH)

    def push(a, b, slot, where):
        pltpu.make_async_remote_copy(
            src_ref=a, dst_ref=b, send_sem=send.at[slot], recv_sem=recv.at[slot],
            device_id=where, device_id_type=pl.DeviceIdType.MESH,
        ).start()

    def drain(ref, sem):
        pltpu.make_async_copy(ref, ref, sem).wait()

    def rows(start, size):
        return pl.ds(pl.multiple_of(start, 8), size)

    barrier = pltpu.get_barrier_semaphore()

    @pl.loop(1, narrow)
    def _(j):
        signal(barrier, x_id(x_peer(j)))

    partners(lambda sp, core: signal(barrier, z_id(sp, core)))

    loads = [
        pltpu.make_async_copy(a, b, loaded.at[n]) for n, (a, b) in enumerate(zip(given, held))
    ]
    first = [0, where_is["fz_hi"], where_is["fz_lo"], where_is["gather"]]
    later = [n for n in range(count) if n not in first]
    for n in first + later:
        loads[n].start()
    before = jnp.where(turn == 0, 0, jnp.where(turn == 1, rep - 1, rep))
    pl.semaphore_wait(barrier, narrow - 1 + (rep - 1) * jnp.minimum(me_sp, 1) + before)

    @pl.when(turn < chips - 1)
    def _():
        for core in range(rep):
            signal(barrier, z_id(turn + 1, core))

    @pl.when(turn == chips - 1)
    def _():
        signal(barrier, z_id(0, 0))

    for n in first:
        loads[n].wait()
    parts = [
        jnp.concatenate([field[128 * c + 32 * x : 128 * c + 32 * x + 32] for c in range(8)], 0)
        for x in range(4)
    ]
    main, packed = forward_z(parts, tabs)
    for c in range(8):
        b1[MSG * c : MSG * c + 32] = main[32 * c : 32 * c + 32]
        b1[MSG * c + 32 : MSG * c + 40] = packed[8 * c : 8 * c + 8]
    for j in far_first(narrow):
        s = x_peer(j)
        push(b1.at[rows(s * MSG, MSG)], r1.at[rows(me_x * MSG, MSG)], 0, x_id(s))

    for y in range(32):
        src[32 * y : 32 * y + 32] = field[pl.ds(y, 32, stride=32)]

    each(0, turn, lambda sp, core: signal(ready.at[me_z], z_id(sp, core)))

    def send_field(sp, core):
        q = sp * rep + core
        push(src.at[rows(q * 32, 32)], fld.at[rows(me_z * 32, 32)], 1, z_id(sp, core))

    def send_modes(sp, core):
        q = sp * rep + core
        push(s3.at[q], n3.at[me_z], 3, z_id(sp, core))

    each(0, turn, send_field)
    partners(send_field)

    r1[rows(me_x * MSG, MSG)] = b1[rows(me_x * MSG, MSG)]
    fld[rows(me_z * 32, 32)] = src[rows(me_z * 32, 32)]
    for n in later:
        loads[n].wait()
    wts[...] = factor_weights(fac_x[...], fac_y[...], fac_z[...], channel, tabs)
    mix_hi[...], mix_lo[...] = split(mix[...])

    near = jnp.minimum(turn + 1 + AHEAD, chips + 1)

    def field_when_ready(sp, core):
        pl.semaphore_wait(ready.at[sp * rep + core], 1)
        send_field(sp, core)

    def both_when_ready(sp, core):
        pl.semaphore_wait(ready.at[sp * rep + core], 1)
        send_modes(sp, core)
        send_field(sp, core)

    each(turn + 1, near, field_when_ready)

    drain(r1.at[pl.ds(0, MSG * (narrow - 1))], recv.at[0])
    blocks = [r1[MSG * s : MSG * s + MSG] for s in range(8)]
    main, extra = spectral_filter(blocks, wts[...], tabs, lane_roll)
    for s in range(8):
        b2[MSG * s : MSG * s + 32] = main[s]
        b2[MSG * s + 32 : MSG * s + 40] = extra[s]

    for j in far_first(narrow):
        s = x_peer(j)
        push(b2.at[rows(s * MSG, MSG)], r2.at[rows(me_x * MSG, MSG)], 2, x_id(s))

    r2[rows(me_x * MSG, MSG)] = b2[rows(me_x * MSG, MSG)]
    drain(r2.at[pl.ds(0, MSG * (narrow - 1))], recv.at[2])
    left = leftover_rows([r2[MSG * c + 32 : MSG * c + 40] for c in range(8)], lane_roll)
    for y in range(32):
        s3[y, :8] = r2[pl.ds(y, 8, stride=MSG)]
        s3[y, 8:] = left[y : y + 1]

    each(0, turn, send_modes)
    partners(send_modes)
    each(turn + 1, near, send_modes)
    each(near, chips + 1, both_when_ready)

    n3[me_z] = s3[me_z]
    drain(n3.at[pl.ds(0, wide - 1)], recv.at[3])
    spectral = inverse_z(
        n3[:, :8].reshape(channels, 128), n3[:, 8:].reshape(wide, 128), (mix_hi[...], mix_lo[...]), tabs
    )
    drain(fld.at[pl.ds(0, 32 * (wide - 1))], recv.at[1])
    first = second = None
    for x in range(4):
        value = spectral[:, 128 * x : 128 * x + 128] + fld[pl.ds(x, channels, stride=4)]
        out[0][x] = value
        first = value if x == 0 else first + value
        second = value * value if x == 0 else second + value * value
    row = stats_row(group_partials(first), group_partials(second))
    st0[0] = row
    ar1[me_z] = row

    for step in far_first(chips):
        sp = me_sp + step
        sp = jnp.where(sp >= chips, sp - chips, sp)
        for core in range(rep):
            push(st0.at[0], ar1.at[me_z], 5, z_id(sp, core))
    for core in range(1, rep):
        push(st0.at[0], ar1.at[me_z], 5, z_id(me_sp, (me_rep + core) % rep))

    drain(ar1.at[pl.ds(0, wide - 1)], recv.at[5])
    row = jnp.sum(ar1[...].reshape(wide, 128), axis=0, keepdims=True)
    st1[0] = row
    ar2[me_x] = row

    for j in far_first(narrow):
        push(st1.at[0], ar2.at[me_x], 6, x_id(x_peer(j)))

    drain(ar2.at[pl.ds(0, narrow - 1)], recv.at[6])
    row = jnp.sum(ar2[...].reshape(narrow, 128), axis=0, keepdims=True)
    out[1][...] = row

    drain(b1.at[pl.ds(0, MSG * (narrow - 1))], send.at[0])
    drain(src.at[pl.ds(0, 32 * (wide - 1))], send.at[1])
    drain(b2.at[pl.ds(0, MSG * (narrow - 1))], send.at[2])
    drain(s3.at[pl.ds(0, wide - 1)], send.at[3])
    drain(ar1.at[pl.ds(0, wide - 1)], send.at[5])
    drain(ar2.at[pl.ds(0, narrow - 1)], send.at[6])


def channel_mlp(count, summed, stats, gain, bias, w_in, b_in, w_out, b_out, out):
    channels = summed.shape[1]
    mean, inv = stats_columns(stats[...], count, channels)
    scale = inv * to_column(gain[...])
    shift, col_in, col_out = (to_column(v[...]) for v in (bias, b_in, b_out))
    wide_in, wide_out = split(w_in[...]), split(w_out[...])
    for x in range(summed.shape[0]):
        value = summed[x]
        normed = (value - mean) * scale + shift
        hidden = gelu(dot3(wide_in, split(normed)) + col_in)
        out[pl.ds(x, channels, stride=4)] = value + dot3(wide_out, split(hidden)) + col_out


def solution(mesh):
    shape = mesh.shape
    wide, narrow = shape["sp"] * shape["rep"], shape["sub"]
    replicated = P()
    placed = (P(("grp", "sp", "rep"), "sub", None, None),) + (replicated,) * 10

    def local(
        field, mix_weight, factor_x, factor_y, factor_z,
        norm_gain, norm_bias, w_in, b_in, w_out, b_out,
    ):
        held, x_local, ny, nz = field.shape
        channels = mix_weight.shape[0]
        nx = x_local * narrow
        kz = factor_z.shape[1]
        tables = build_tables(nx, ny, nz, kz, held, wide)
        sizes = dict(
            wide=wide, narrow=narrow, channels=channels, rep=shape["rep"],
            count=GROUP_CHANNELS * nx * ny * nz,
        )
        row = lambda v: v.reshape(1, -1)
        operands = [
            field.reshape(held * x_local * ny, nz), factor_x.T, factor_y.T, factor_z.T, mix_weight,
        ] + [jnp.asarray(tables[name]) for name in TABLES]
        cells = channels * x_local
        vmem = pl.BlockSpec(memory_space=pltpu.VMEM)
        f32 = lambda *dims: pltpu.VMEM(dims, F32)
        b16 = lambda *dims: pltpu.VMEM(dims, BF16)
        square = (channels, channels)
        summed, stats = pl.pallas_call(
            lambda *refs: fused(sizes, *refs),
            out_shape=(
                jax.ShapeDtypeStruct((x_local, channels, nz), F32),
                jax.ShapeDtypeStruct((1, 128), F32),
            ),
            in_specs=[pl.BlockSpec(memory_space=pltpu.HBM)] * len(operands),
            out_specs=(vmem, vmem),
            scratch_shapes=[pltpu.VMEM(v.shape, v.dtype) for v in operands]
            + [pltpu.SemaphoreType.DMA((len(operands),))]
            + [
                f32(cells, nz), f32(cells, nz),
                f32(MSG * narrow, 128), f32(MSG * narrow, 128),
                f32(MSG * narrow, 128), f32(MSG * narrow, 128),
                f32(wide, 9, 128), f32(wide, 9, 128),
                f32(1, 1, 128), f32(wide, 1, 128), f32(1, 1, 128), f32(narrow, 1, 128),
                f32(ny, 9 * 128),
                b16(*square), b16(*square),
                pltpu.SemaphoreType.DMA((7,)), pltpu.SemaphoreType.DMA((7,)),
                pltpu.SemaphoreType.REGULAR((wide,)),
            ],
            compiler_params=pltpu.CompilerParams(
                collective_id=0, has_side_effects=True, vmem_limit_bytes=24 * 2**20
            ),
        )(*[pltpu.with_memory_space_constraint(v, pltpu.HBM) for v in operands])
        result = pl.pallas_call(
            functools.partial(channel_mlp, sizes["count"]),
            out_shape=jax.ShapeDtypeStruct((cells, nz), F32),
            in_specs=[vmem] * 8,
            out_specs=vmem,
            compiler_params=pltpu.CompilerParams(vmem_limit_bytes=24 * 2**20),
        )(summed, stats, row(norm_gain), row(norm_bias), w_in, row(b_in), w_out, row(b_out))
        return result.reshape(channels, x_local, 1, nz)

    return jax.shard_map(
        local,
        mesh=mesh,
        in_specs=placed,
        out_specs=P("grp", "sub", ("sp", "rep"), None),
        check_vma=False,
    )
```

```python
import functools
import math

import jax
import jax.numpy as jnp
import numpy as np
from jax import lax
from jax.experimental import pallas as pl
from jax.experimental.pallas import tpu as pltpu
from jax.sharding import PartitionSpec as P

F32 = jnp.float32
BF16 = jnp.bfloat16
GROUP_CHANNELS = 8
EPS = 1e-05


def split_np(a):
    a = np.asarray(a, np.float32)
    hi = a.astype(BF16)
    lo = (a - hi.astype(np.float32)).astype(BF16)
    return hi, lo


def build_tables(nx, ny, nz, kz, ch_local, wide):
    xl = 4
    chunks = 8
    lane = np.arange(128)
    k_of, x_of, r_of = lane // 16, (lane // 4) % 4, lane % 4
    z = np.arange(nz)
    scale = 1.0 / (nx * ny * nz)
    top = kz // 2
    fwd_z = np.zeros((xl, nz, 256))
    inv_z = np.zeros((256, xl, nz))
    for l in range(128):
        f = 2 * k_of[l] + r_of[l] // 2
        ang = 2 * np.pi * ((f * z) % nz) / nz
        fwd_z[x_of[l], :, l] = (np.cos(ang) if r_of[l] % 2 == 0 else -np.sin(ang)) * scale
        inv_z[l, x_of[l], :] = np.cos(ang) if r_of[l] % 2 == 0 else -np.sin(ang)
        if r_of[l] < 2:
            ang = 2 * np.pi * ((top * z) % nz) / nz
            col = np.cos(ang) if r_of[l] == 0 else -np.sin(ang)
            fwd_z[x_of[l], :, 128 + l] = col * scale
            inv_z[128 + l, x_of[l], :] = col
    fwd_z = fwd_z.reshape(xl * nz, 256)
    inv_z = inv_z.reshape(256, xl * nz)
    ax = np.arange(nx)
    ang = 2 * np.pi * ((ax[:, None] * ax[None, :]) % nx) / nx
    c, s = np.cos(ang), np.sin(ang)
    fwd = np.zeros((nx, 2, 2, nx, 2, 2))
    inv = np.zeros((nx, 2, 2, nx, 2, 2))
    for f in range(2):
        fwd[:, f, 0, :, f, 0] = c
        fwd[:, f, 1, :, f, 0] = s
        fwd[:, f, 0, :, f, 1] = -s
        fwd[:, f, 1, :, f, 1] = c
        inv[:, f, 0, :, f, 0] = c
        inv[:, f, 1, :, f, 0] = -s
        inv[:, f, 0, :, f, 1] = s
        inv[:, f, 1, :, f, 1] = c
    turn = np.zeros((128, 128))
    for l in range(0, 128, 2):
        turn[l + 1, l] = 1.0
        turn[l, l + 1] = -1.0
    fwd = fwd.reshape(128, 128)
    inv = inv.reshape(128, 128)
    x_fwd = np.concatenate([fwd, fwd @ turn], 1)
    x_inv = np.concatenate([inv, -(inv @ turn)], 1)
    ay = np.arange(ny)
    ang = 2 * np.pi * ((ay[:, None] * ay[None, :]) % ny) / ny
    y_tab = np.concatenate([np.cos(ang), np.sin(ang)], 1)
    hi, lo = split_np(y_tab)
    y_tab3 = np.concatenate([hi, hi, lo], 1)
    sel_x = np.zeros((nx, 256))
    for a in range(nx):
        sel_x[a, 4 * a : 4 * a + 4] = 1.0
        sel_x[a, 128 + 4 * ((nx - a) % nx) : 128 + 4 * ((nx - a) % nx) + 4] = 1.0
    sel_z = np.zeros((kz, 2, 9, nx, 4))
    for f in range(top + 1):
        k, f2 = f // 2, f % 2
        if f < top:
            sel_z[f, 0, k, :, 2 * f2 : 2 * f2 + 2] = 1.0
        if f > 0:
            sel_z[kz - f, 1, k, :, 2 * f2 : 2 * f2 + 2] = 1.0
    sel_z = sel_z.reshape(kz, 2 * 9 * 128)
    rows_in = np.arange(ch_local * ny)
    rows_out = np.arange(ch_local * 8)
    gather = (
        (rows_in[None, :] // ny == rows_out[:, None] // 8)
        & (rows_in[None, :] % 8 == rows_out[:, None] % 8)
    ).astype(np.float32)
    rows_all = np.arange(ch_local * wide)
    spread = (rows_all[:, None] // ch_local == np.arange(wide)[None, :]).astype(np.float32)
    fz = split_np(fwd_z)
    iz = split_np(inv_z)
    xf = split_np(x_fwd)
    xi = split_np(x_inv)
    return dict(
        fz_hi=fz[0], fz_lo=fz[1], iz_hi=iz[0], iz_lo=iz[1],
        xf_hi=xf[0], xf_lo=xf[1], xi_hi=xi[0], xi_lo=xi[1],
        y_tab=y_tab3,
        sel_x=sel_x.astype(np.float32), sel_z=sel_z.astype(np.float32),
        gather=gather.astype(BF16), spread=spread.astype(BF16),
    )


def split(a):
    hi = a.astype(BF16)
    return hi, (a - hi.astype(F32)).astype(BF16)


def dot1(a, b):
    return lax.dot_general(a, b, (((1,), (0,)), ((), ())), preferred_element_type=F32)


def dot3(a, b):
    return dot1(a[0], b[0]) + dot1(a[0], b[1]) + dot1(a[1], b[0])


def swap_chunks(arrays, roll):
    arrays = list(arrays)
    rows = arrays[0].shape[0]
    chunk = lax.broadcasted_iota(jnp.int32, (rows, 128), 1) // 16
    for d in (4, 2, 1):
        upper = (chunk // d) % 2 == 1
        for i in range(8):
            if (i // d) % 2 == 0:
                low, high = arrays[i], arrays[i + d]
                arrays[i] = jnp.where(upper, roll(high, 16 * d), low)
                arrays[i + d] = jnp.where(upper, high, roll(low, 128 - 16 * d))
    return arrays


def forward_z(parts, tabs):
    fz_hi, fz_lo = tabs["fz_hi"], tabs["fz_lo"]
    total = None
    for x, part in enumerate(parts):
        term = dot3(split(part), (fz_hi[128 * x : 128 * x + 128], fz_lo[128 * x : 128 * x + 128]))
        total = term if total is None else total + term
    main, extra = total[:, :128], total[:, 128:]
    rows, lanes = (lax.broadcasted_iota(jnp.int32, extra.shape, d) for d in (0, 1))
    extra = jnp.where((rows % 32) // 8 == lanes // 16, extra, 0.0)
    hi, lo = split(extra)
    packed = dot1(tabs["gather"], hi) + dot1(tabs["gather"], lo)
    return main, packed


def factor_weights(fac_x, fac_y, fac_z, channel, tabs):
    n, channels = fac_y.shape
    own = lax.broadcasted_iota(jnp.int32, (n, channels), 1) == channel
    col_x, col_y, col_z = (
        jnp.sum(jnp.where(own, f, 0.0), axis=1, keepdims=True) for f in (fac_x, fac_y, fac_z)
    )
    lanes_x = jnp.sum(col_x * tabs["sel_x"], axis=0, keepdims=True)
    lanes_z = jnp.sum(col_z * tabs["sel_z"], axis=0, keepdims=True)
    plus = lanes_z[:, :1152] * jnp.concatenate([lanes_x[:, :128]] * 9, 1)
    minus = lanes_z[:, 1152:] * jnp.concatenate([lanes_x[:, 128:]] * 9, 1)
    r, c = (lax.broadcasted_iota(jnp.int32, (n, n), d) for d in (0, 1))
    row_y = jnp.sum(jnp.where(r == c, col_y, 0.0), axis=0, keepdims=True)
    flipped = jnp.where((n - r) % n == c, jnp.broadcast_to(row_y, (n, n)), 0.0)
    col_minus = jnp.sum(flipped, axis=1, keepdims=True)
    return col_y * plus + col_minus * minus


def spectral_filter(blocks, weights, tabs, roll):
    main = swap_chunks([b[:32] for b in blocks], roll)
    extra = swap_chunks([b[32:40] for b in blocks], roll)
    last = jnp.concatenate(extra[:4], 0)
    rows = jnp.concatenate(main + [last], 0)

    def along_y(pairs):
        stacked = jnp.concatenate(
            [
                jnp.concatenate(
                    [pairs[32 * k : 32 * k + 32, :128], pairs[32 * k : 32 * k + 32, 128:]], 0
                )
                for k in range(9)
            ],
            1,
        )
        hi, lo = split(stacked)
        return dot1(tabs["y_tab"], jnp.concatenate([hi, lo, hi], 0))

    pairs = dot3(split(rows), (tabs["xf_hi"], tabs["xf_lo"]))
    spec = along_y(pairs) * weights
    rows = jnp.concatenate([spec[:, 128 * k : 128 * k + 128] for k in range(9)], 0)
    pairs = dot3(split(rows), (tabs["xi_hi"], tabs["xi_lo"]))
    back = along_y(pairs)
    main = swap_chunks([back[:, 128 * k : 128 * k + 128] for k in range(8)], roll)
    last = back[:, 1024:]
    tiles = [last[8 * p : 8 * p + 8] for p in range(4)] + [jnp.zeros((8, 128), F32)] * 4
    extra = swap_chunks(tiles, roll)
    return main, extra


def leftover_rows(extras, roll):
    return jnp.concatenate(swap_chunks(extras, roll)[:4], 0)


def inverse_z(modes, left, mix, tabs):
    hi, lo = split(left)
    wide = dot1(tabs["spread"], hi) + dot1(tabs["spread"], lo)
    rows, lanes = (lax.broadcasted_iota(jnp.int32, wide.shape, d) for d in (0, 1))
    wide = jnp.where(rows % 8 == lanes // 16, wide, 0.0)
    both = jnp.concatenate([modes, wide], 1)
    mixed = dot3(mix, split(both))
    return dot3(split(mixed), (tabs["iz_hi"], tabs["iz_lo"]))


def to_column(row):
    n = row.shape[1]
    r, c = (lax.broadcasted_iota(jnp.int32, (n, n), d) for d in (0, 1))
    return jnp.sum(jnp.where(r == c, jnp.broadcast_to(row, (n, n)), 0.0), axis=1, keepdims=True)


def group_partials(total):
    folded = jnp.sum(total.reshape(total.shape[0] // 8, 8, 128), axis=1)
    return jnp.sum(folded, axis=1, keepdims=True)


def stats_row(first, second):
    n = first.shape[0]
    r, c = (lax.broadcasted_iota(jnp.int32, (n, 128), d) for d in (0, 1))
    placed = jnp.where(r == c, first, 0.0) + jnp.where(r + n == c, second, 0.0)
    return jnp.sum(placed, axis=0, keepdims=True)


def stats_columns(row, count, channels):
    groups = channels // GROUP_CHANNELS
    r, c = (lax.broadcasted_iota(jnp.int32, (channels, 128), d) for d in (0, 1))
    wide = jnp.broadcast_to(row, (channels, 128))
    first = jnp.sum(jnp.where(r // GROUP_CHANNELS == c, wide, 0.0), axis=1, keepdims=True)
    second = jnp.sum(
        jnp.where(r // GROUP_CHANNELS + groups == c, wide, 0.0), axis=1, keepdims=True
    )
    mean = first / count
    var = second / count - mean * mean
    return mean, lax.rsqrt(var + EPS)


def gelu(v):
    inner = math.sqrt(2.0 / math.pi) * (v + 0.044715 * (v * v * v))
    return 0.5 * v * (1.0 + jnp.tanh(inner))


TABLES = (
    "fz_hi", "fz_lo", "iz_hi", "iz_lo", "xf_hi", "xf_lo", "xi_hi", "xi_lo",
    "y_tab", "sel_x", "sel_z", "gather", "spread",
)
MSG = 40


class Lazy:
    def __init__(self, refs):
        self.refs = refs

    def __getitem__(self, name):
        return self.refs[name][...]


def lane_roll(a, shift):
    return pltpu.roll(a, shift, axis=1)


def far_first(n):
    return sorted(range(1, n), key=lambda d: -min(d, n - d))


AHEAD = 4


def fused(sizes, *refs):
    wide, narrow, channels = sizes["wide"], sizes["narrow"], sizes["channels"]
    rep = sizes["rep"]
    count = 5 + len(TABLES)
    given, out = refs[:count], refs[count : count + 2]
    scratch = refs[count + 2 :]
    held, loaded, scratch = scratch[:count], scratch[count], scratch[count + 1 :]
    (field, fac_x, fac_y, fac_z, mix) = held[:5]
    tabs = Lazy(dict(zip(TABLES, held[5:])))
    where_is = {name: 5 + n for n, name in enumerate(TABLES)}
    (
        src, fld, b1, r1, b2, r2, s3, n3, st0, ar1, st1, ar2,
        wts, mix_hi, mix_lo, send, recv, ready,
    ) = scratch
    me_x, me_sp, me_rep = lax.axis_index("sub"), lax.axis_index("sp"), lax.axis_index("rep")
    me_z = me_sp * rep + me_rep
    channel = me_z * narrow + me_x
    chips = wide // rep
    last = (me_sp == 0) & (me_rep == 0)
    turn = jnp.where(last, chips, me_sp)

    def each(low, high, action):
        @pl.loop(low, high)
        def _(position):
            sp = jnp.where(position == chips, 0, position)
            for core in range(rep):

                @pl.when(position > 0 if core == 0 else position < chips)
                def _():
                    action(sp, core)

    def partners(action):
        @pl.when(me_sp > 0)
        def _():
            for core in range(1, rep):
                action(me_sp, (me_rep + core) % rep)

    def z_id(sp, core):
        return {"sp": sp, "rep": core}

    def x_id(s):
        return {"sub": s}

    def x_peer(j):
        s = me_x + j
        return jnp.where(s >= narrow, s - narrow, s)

    def signal(sem, where):
        pl.semaphore_signal(sem, inc=1, device_id=where, device_id_type=pl.DeviceIdType.MESH)

    def push(a, b, slot, where):
        pltpu.make_async_remote_copy(
            src_ref=a, dst_ref=b, send_sem=send.at[slot], recv_sem=recv.at[slot],
            device_id=where, device_id_type=pl.DeviceIdType.MESH,
        ).start()

    def drain(ref, sem):
        pltpu.make_async_copy(ref, ref, sem).wait()

    def rows(start, size):
        return pl.ds(pl.multiple_of(start, 8), size)

    barrier = pltpu.get_barrier_semaphore()

    @pl.loop(1, narrow)
    def _(j):
        signal(barrier, x_id(x_peer(j)))

    partners(lambda sp, core: signal(barrier, z_id(sp, core)))

    loads = [
        pltpu.make_async_copy(a, b, loaded.at[n]) for n, (a, b) in enumerate(zip(given, held))
    ]
    first = [0, where_is["fz_hi"], where_is["fz_lo"], where_is["gather"]]
    later = [n for n in range(count) if n not in first]
    for n in first + later:
        loads[n].start()
    def own_modes(waits):
        for n in waits:
            loads[n].wait()
        parts = [
            jnp.concatenate([field[128 * c + 32 * x : 128 * c + 32 * x + 32] for c in range(8)], 0)
            for x in range(4)
        ]
        main, packed = forward_z(parts, tabs)
        for c in range(8):
            b1[MSG * c : MSG * c + 32] = main[32 * c : 32 * c + 32]
            b1[MSG * c + 32 : MSG * c + 40] = packed[8 * c : 8 * c + 8]

    pl.when(turn == chips)(lambda: own_modes(first))

    before = jnp.where(turn == 0, 0, jnp.where(turn == 1, rep - 1, rep))
    pl.semaphore_wait(barrier, narrow - 1 + (rep - 1) * jnp.minimum(me_sp, 1) + before)

    @pl.when(turn < chips - 1)
    def _():
        for core in range(rep):
            signal(barrier, z_id(turn + 1, core))

    @pl.when(turn == chips - 1)
    def _():
        signal(barrier, z_id(0, 0))

    def send_field(sp, core):
        q = sp * rep + core
        push(src.at[rows(q * 32, 32)], fld.at[rows(me_z * 32, 32)], 1, z_id(sp, core))

    def spread_field():
        for y in range(32):
            src[32 * y : 32 * y + 32] = field[pl.ds(y, 32, stride=32)]
        each(0, turn, send_field)
        partners(send_field)

    def tell_before():
        each(0, turn, lambda sp, core: signal(ready.at[me_z], z_id(sp, core)))

    @pl.when(turn < chips)
    def _():
        tell_before()
        for n in first[:1]:
            loads[n].wait()
        pl.when(turn < chips - 1)(spread_field)
        own_modes(first[1:])

    for j in far_first(narrow):
        s = x_peer(j)
        push(b1.at[rows(s * MSG, MSG)], r1.at[rows(me_x * MSG, MSG)], 0, x_id(s))

    def send_modes(sp, core):
        q = sp * rep + core
        push(s3.at[q], n3.at[me_z], 3, z_id(sp, core))

    pl.when(turn == chips)(tell_before)
    pl.when(turn >= chips - 1)(spread_field)

    r1[rows(me_x * MSG, MSG)] = b1[rows(me_x * MSG, MSG)]
    fld[rows(me_z * 32, 32)] = src[rows(me_z * 32, 32)]
    for n in later:
        loads[n].wait()
    wts[...] = factor_weights(fac_x[...], fac_y[...], fac_z[...], channel, tabs)
    mix_hi[...], mix_lo[...] = split(mix[...])

    near = jnp.minimum(turn + 1 + AHEAD, chips + 1)

    def field_when_ready(sp, core):
        pl.semaphore_wait(ready.at[sp * rep + core], 1)
        send_field(sp, core)

    def both_when_ready(sp, core):
        pl.semaphore_wait(ready.at[sp * rep + core], 1)
        send_modes(sp, core)
        send_field(sp, core)

    each(turn + 1, near, field_when_ready)

    drain(r1.at[pl.ds(0, MSG * (narrow - 1))], recv.at[0])
    blocks = [r1[MSG * s : MSG * s + MSG] for s in range(8)]
    main, extra = spectral_filter(blocks, wts[...], tabs, lane_roll)
    for s in range(8):
        b2[MSG * s : MSG * s + 32] = main[s]
        b2[MSG * s + 32 : MSG * s + 40] = extra[s]

    for j in far_first(narrow):
        s = x_peer(j)
        push(b2.at[rows(s * MSG, MSG)], r2.at[rows(me_x * MSG, MSG)], 2, x_id(s))

    r2[rows(me_x * MSG, MSG)] = b2[rows(me_x * MSG, MSG)]
    drain(r2.at[pl.ds(0, MSG * (narrow - 1))], recv.at[2])
    left = leftover_rows([r2[MSG * c + 32 : MSG * c + 40] for c in range(8)], lane_roll)
    for y in range(32):
        s3[y, :8] = r2[pl.ds(y, 8, stride=MSG)]
        s3[y, 8:] = left[y : y + 1]

    @pl.when(near == chips + 1)
    def _():
        for step in far_first(chips):
            sp = me_sp + step
            for core in range(rep):
                send_modes(jnp.where(sp >= chips, sp - chips, sp), core)
        for core in range(1, rep):
            send_modes(me_sp, (me_rep + core) % rep)

    @pl.when(near < chips + 1)
    def _():
        each(0, turn, send_modes)
        partners(send_modes)
        each(turn + 1, near, send_modes)
        each(near, chips + 1, both_when_ready)

    n3[me_z] = s3[me_z]
    drain(n3.at[pl.ds(0, wide - 1)], recv.at[3])
    spectral = inverse_z(
        n3[:, :8].reshape(channels, 128), n3[:, 8:].reshape(wide, 128), (mix_hi[...], mix_lo[...]), tabs
    )
    drain(fld.at[pl.ds(0, 32 * (wide - 1))], recv.at[1])
    first = second = None
    for x in range(4):
        value = spectral[:, 128 * x : 128 * x + 128] + fld[pl.ds(x, channels, stride=4)]
        out[0][x] = value
        first = value if x == 0 else first + value
        second = value * value if x == 0 else second + value * value
    row = stats_row(group_partials(first), group_partials(second))
    st0[0] = row
    ar1[me_z] = row

    for step in far_first(chips):
        sp = me_sp + step
        sp = jnp.where(sp >= chips, sp - chips, sp)
        for core in range(rep):
            push(st0.at[0], ar1.at[me_z], 5, z_id(sp, core))
    for core in range(1, rep):
        push(st0.at[0], ar1.at[me_z], 5, z_id(me_sp, (me_rep + core) % rep))

    drain(ar1.at[pl.ds(0, wide - 1)], recv.at[5])
    row = jnp.sum(ar1[...].reshape(wide, 128), axis=0, keepdims=True)
    st1[0] = row
    ar2[me_x] = row

    for j in far_first(narrow):
        push(st1.at[0], ar2.at[me_x], 6, x_id(x_peer(j)))

    drain(ar2.at[pl.ds(0, narrow - 1)], recv.at[6])
    row = jnp.sum(ar2[...].reshape(narrow, 128), axis=0, keepdims=True)
    out[1][...] = row

    drain(b1.at[pl.ds(0, MSG * (narrow - 1))], send.at[0])
    drain(src.at[pl.ds(0, 32 * (wide - 1))], send.at[1])
    drain(b2.at[pl.ds(0, MSG * (narrow - 1))], send.at[2])
    drain(s3.at[pl.ds(0, wide - 1)], send.at[3])
    drain(ar1.at[pl.ds(0, wide - 1)], send.at[5])
    drain(ar2.at[pl.ds(0, narrow - 1)], send.at[6])


def channel_mlp(count, summed, stats, gain, bias, w_in, b_in, w_out, b_out, out):
    channels = summed.shape[1]
    mean, inv = stats_columns(stats[...], count, channels)
    scale = inv * to_column(gain[...])
    shift, col_in, col_out = (to_column(v[...]) for v in (bias, b_in, b_out))
    wide_in, wide_out = split(w_in[...]), split(w_out[...])
    for x in range(summed.shape[0]):
        value = summed[x]
        normed = (value - mean) * scale + shift
        hidden = gelu(dot3(wide_in, split(normed)) + col_in)
        out[pl.ds(x, channels, stride=4)] = value + dot3(wide_out, split(hidden)) + col_out


def solution(mesh):
    shape = mesh.shape
    wide, narrow = shape["sp"] * shape["rep"], shape["sub"]
    replicated = P()
    placed = (P(("grp", "sp", "rep"), "sub", None, None),) + (replicated,) * 10

    def local(
        field, mix_weight, factor_x, factor_y, factor_z,
        norm_gain, norm_bias, w_in, b_in, w_out, b_out,
    ):
        held, x_local, ny, nz = field.shape
        channels = mix_weight.shape[0]
        nx = x_local * narrow
        kz = factor_z.shape[1]
        tables = build_tables(nx, ny, nz, kz, held, wide)
        sizes = dict(
            wide=wide, narrow=narrow, channels=channels, rep=shape["rep"],
            count=GROUP_CHANNELS * nx * ny * nz,
        )
        row = lambda v: v.reshape(1, -1)
        operands = [
            field.reshape(held * x_local * ny, nz), factor_x.T, factor_y.T, factor_z.T, mix_weight,
        ] + [jnp.asarray(tables[name]) for name in TABLES]
        cells = channels * x_local
        vmem = pl.BlockSpec(memory_space=pltpu.VMEM)
        f32 = lambda *dims: pltpu.VMEM(dims, F32)
        b16 = lambda *dims: pltpu.VMEM(dims, BF16)
        square = (channels, channels)
        summed, stats = pl.pallas_call(
            lambda *refs: fused(sizes, *refs),
            out_shape=(
                jax.ShapeDtypeStruct((x_local, channels, nz), F32),
                jax.ShapeDtypeStruct((1, 128), F32),
            ),
            in_specs=[pl.BlockSpec(memory_space=pltpu.HBM)] * len(operands),
            out_specs=(vmem, vmem),
            scratch_shapes=[pltpu.VMEM(v.shape, v.dtype) for v in operands]
            + [pltpu.SemaphoreType.DMA((len(operands),))]
            + [
                f32(cells, nz), f32(cells, nz),
                f32(MSG * narrow, 128), f32(MSG * narrow, 128),
                f32(MSG * narrow, 128), f32(MSG * narrow, 128),
                f32(wide, 9, 128), f32(wide, 9, 128),
                f32(1, 1, 128), f32(wide, 1, 128), f32(1, 1, 128), f32(narrow, 1, 128),
                f32(ny, 9 * 128),
                b16(*square), b16(*square),
                pltpu.SemaphoreType.DMA((7,)), pltpu.SemaphoreType.DMA((7,)),
                pltpu.SemaphoreType.REGULAR((wide,)),
            ],
            compiler_params=pltpu.CompilerParams(
                collective_id=0, has_side_effects=True, vmem_limit_bytes=24 * 2**20
            ),
        )(*[pltpu.with_memory_space_constraint(v, pltpu.HBM) for v in operands])
        result = pl.pallas_call(
            functools.partial(channel_mlp, sizes["count"]),
            out_shape=jax.ShapeDtypeStruct((cells, nz), F32),
            in_specs=[vmem] * 8,
            out_specs=vmem,
            compiler_params=pltpu.CompilerParams(vmem_limit_bytes=24 * 2**20),
        )(summed, stats, row(norm_gain), row(norm_bias), w_in, row(b_in), w_out, row(b_out))
        return result.reshape(channels, x_local, 1, nz)

    return jax.shard_map(
        local,
        mesh=mesh,
        in_specs=placed,
        out_specs=P("grp", "sub", ("sp", "rep"), None),
        check_vma=False,
    )
```

```python
import functools
import math

import jax
import jax.numpy as jnp
import numpy as np
from jax import lax
from jax.experimental import pallas as pl
from jax.experimental.pallas import tpu as pltpu
from jax.sharding import PartitionSpec as P

F32 = jnp.float32
BF16 = jnp.bfloat16
GROUP_CHANNELS = 8
EPS = 1e-05


def split_np(a):
    a = np.asarray(a, np.float32)
    hi = a.astype(BF16)
    lo = (a - hi.astype(np.float32)).astype(BF16)
    return hi, lo


def build_tables(nx, ny, nz, kz, ch_local, wide):
    xl = 4
    chunks = 8
    lane = np.arange(128)
    k_of, x_of, r_of = lane // 16, (lane // 4) % 4, lane % 4
    z = np.arange(nz)
    scale = 1.0 / (nx * ny * nz)
    top = kz // 2
    fwd_z = np.zeros((xl, nz, 256))
    inv_z = np.zeros((256, xl, nz))
    for l in range(128):
        f = 2 * k_of[l] + r_of[l] // 2
        ang = 2 * np.pi * ((f * z) % nz) / nz
        fwd_z[x_of[l], :, l] = (np.cos(ang) if r_of[l] % 2 == 0 else -np.sin(ang)) * scale
        inv_z[l, x_of[l], :] = np.cos(ang) if r_of[l] % 2 == 0 else -np.sin(ang)
        if r_of[l] < 2:
            ang = 2 * np.pi * ((top * z) % nz) / nz
            col = np.cos(ang) if r_of[l] == 0 else -np.sin(ang)
            fwd_z[x_of[l], :, 128 + l] = col * scale
            inv_z[128 + l, x_of[l], :] = col
    fwd_z = fwd_z.reshape(xl * nz, 256)
    inv_z = inv_z.reshape(256, xl * nz)
    ax = np.arange(nx)
    ang = 2 * np.pi * ((ax[:, None] * ax[None, :]) % nx) / nx
    c, s = np.cos(ang), np.sin(ang)
    fwd = np.zeros((nx, 2, 2, nx, 2, 2))
    inv = np.zeros((nx, 2, 2, nx, 2, 2))
    for f in range(2):
        fwd[:, f, 0, :, f, 0] = c
        fwd[:, f, 1, :, f, 0] = s
        fwd[:, f, 0, :, f, 1] = -s
        fwd[:, f, 1, :, f, 1] = c
        inv[:, f, 0, :, f, 0] = c
        inv[:, f, 1, :, f, 0] = -s
        inv[:, f, 0, :, f, 1] = s
        inv[:, f, 1, :, f, 1] = c
    turn = np.zeros((128, 128))
    for l in range(0, 128, 2):
        turn[l + 1, l] = 1.0
        turn[l, l + 1] = -1.0
    fwd = fwd.reshape(128, 128)
    inv = inv.reshape(128, 128)
    x_fwd = np.concatenate([fwd, fwd @ turn], 1)
    x_inv = np.concatenate([inv, -(inv @ turn)], 1)
    ay = np.arange(ny)
    ang = 2 * np.pi * ((ay[:, None] * ay[None, :]) % ny) / ny
    y_tab = np.concatenate([np.cos(ang), np.sin(ang)], 1)
    hi, lo = split_np(y_tab)
    y_tab3 = np.concatenate([hi, hi, lo], 1)
    sel_x = np.zeros((nx, 256))
    for a in range(nx):
        sel_x[a, 4 * a : 4 * a + 4] = 1.0
        sel_x[a, 128 + 4 * ((nx - a) % nx) : 128 + 4 * ((nx - a) % nx) + 4] = 1.0
    sel_z = np.zeros((kz, 2, 9, nx, 4))
    for f in range(top + 1):
        k, f2 = f // 2, f % 2
        if f < top:
            sel_z[f, 0, k, :, 2 * f2 : 2 * f2 + 2] = 1.0
        if f > 0:
            sel_z[kz - f, 1, k, :, 2 * f2 : 2 * f2 + 2] = 1.0
    sel_z = sel_z.reshape(kz, 2 * 9 * 128)
    rows_in = np.arange(ch_local * ny)
    rows_out = np.arange(ch_local * 8)
    gather = (
        (rows_in[None, :] // ny == rows_out[:, None] // 8)
        & (rows_in[None, :] % 8 == rows_out[:, None] % 8)
    ).astype(np.float32)
    rows_all = np.arange(ch_local * wide)
    spread = (rows_all[:, None] // ch_local == np.arange(wide)[None, :]).astype(np.float32)
    fz = split_np(fwd_z)
    iz = split_np(inv_z)
    xf = split_np(x_fwd)
    xi = split_np(x_inv)
    return dict(
        fz_hi=fz[0], fz_lo=fz[1], iz_hi=iz[0], iz_lo=iz[1],
        xf_hi=xf[0], xf_lo=xf[1], xi_hi=xi[0], xi_lo=xi[1],
        y_tab=y_tab3,
        sel_x=sel_x.astype(np.float32), sel_z=sel_z.astype(np.float32),
        gather=gather.astype(BF16), spread=spread.astype(BF16),
    )


def split(a):
    hi = a.astype(BF16)
    return hi, (a - hi.astype(F32)).astype(BF16)


def dot1(a, b):
    return lax.dot_general(a, b, (((1,), (0,)), ((), ())), preferred_element_type=F32)


def dot3(a, b):
    return dot1(a[0], b[0]) + dot1(a[0], b[1]) + dot1(a[1], b[0])


def swap_chunks(arrays, roll):
    arrays = list(arrays)
    rows = arrays[0].shape[0]
    chunk = lax.broadcasted_iota(jnp.int32, (rows, 128), 1) // 16
    for d in (4, 2, 1):
        upper = (chunk // d) % 2 == 1
        for i in range(8):
            if (i // d) % 2 == 0:
                low, high = arrays[i], arrays[i + d]
                arrays[i] = jnp.where(upper, roll(high, 16 * d), low)
                arrays[i + d] = jnp.where(upper, high, roll(low, 128 - 16 * d))
    return arrays


def forward_z(parts, tabs):
    fz_hi, fz_lo = tabs["fz_hi"], tabs["fz_lo"]
    total = None
    for x, part in enumerate(parts):
        term = dot3(split(part), (fz_hi[128 * x : 128 * x + 128], fz_lo[128 * x : 128 * x + 128]))
        total = term if total is None else total + term
    main, extra = total[:, :128], total[:, 128:]
    rows, lanes = (lax.broadcasted_iota(jnp.int32, extra.shape, d) for d in (0, 1))
    extra = jnp.where((rows % 32) // 8 == lanes // 16, extra, 0.0)
    hi, lo = split(extra)
    packed = dot1(tabs["gather"], hi) + dot1(tabs["gather"], lo)
    return main, packed


def factor_weights(fac_x, fac_y, fac_z, channel, tabs):
    n, channels = fac_y.shape
    own = lax.broadcasted_iota(jnp.int32, (n, channels), 1) == channel
    col_x, col_y, col_z = (
        jnp.sum(jnp.where(own, f, 0.0), axis=1, keepdims=True) for f in (fac_x, fac_y, fac_z)
    )
    lanes_x = jnp.sum(col_x * tabs["sel_x"], axis=0, keepdims=True)
    lanes_z = jnp.sum(col_z * tabs["sel_z"], axis=0, keepdims=True)
    plus = lanes_z[:, :1152] * jnp.concatenate([lanes_x[:, :128]] * 9, 1)
    minus = lanes_z[:, 1152:] * jnp.concatenate([lanes_x[:, 128:]] * 9, 1)
    r, c = (lax.broadcasted_iota(jnp.int32, (n, n), d) for d in (0, 1))
    row_y = jnp.sum(jnp.where(r == c, col_y, 0.0), axis=0, keepdims=True)
    flipped = jnp.where((n - r) % n == c, jnp.broadcast_to(row_y, (n, n)), 0.0)
    col_minus = jnp.sum(flipped, axis=1, keepdims=True)
    return col_y * plus + col_minus * minus


def spectral_filter(blocks, weights, tabs, roll):
    main = swap_chunks([b[:32] for b in blocks], roll)
    extra = swap_chunks([b[32:40] for b in blocks], roll)
    last = jnp.concatenate(extra[:4], 0)
    rows = jnp.concatenate(main + [last], 0)

    def along_y(pairs):
        stacked = jnp.concatenate(
            [
                jnp.concatenate(
                    [pairs[32 * k : 32 * k + 32, :128], pairs[32 * k : 32 * k + 32, 128:]], 0
                )
                for k in range(9)
            ],
            1,
        )
        hi, lo = split(stacked)
        return dot1(tabs["y_tab"], jnp.concatenate([hi, lo, hi], 0))

    pairs = dot3(split(rows), (tabs["xf_hi"], tabs["xf_lo"]))
    spec = along_y(pairs) * weights
    rows = jnp.concatenate([spec[:, 128 * k : 128 * k + 128] for k in range(9)], 0)
    pairs = dot3(split(rows), (tabs["xi_hi"], tabs["xi_lo"]))
    back = along_y(pairs)
    main = swap_chunks([back[:, 128 * k : 128 * k + 128] for k in range(8)], roll)
    last = back[:, 1024:]
    tiles = [last[8 * p : 8 * p + 8] for p in range(4)] + [jnp.zeros((8, 128), F32)] * 4
    extra = swap_chunks(tiles, roll)
    return main, extra


def leftover_rows(extras, roll):
    return jnp.concatenate(swap_chunks(extras, roll)[:4], 0)


def inverse_z(modes, left, mix, tabs):
    hi, lo = split(left)
    wide = dot1(tabs["spread"], hi) + dot1(tabs["spread"], lo)
    rows, lanes = (lax.broadcasted_iota(jnp.int32, wide.shape, d) for d in (0, 1))
    wide = jnp.where(rows % 8 == lanes // 16, wide, 0.0)
    both = jnp.concatenate([modes, wide], 1)
    mixed = dot3(mix, split(both))
    return dot3(split(mixed), (tabs["iz_hi"], tabs["iz_lo"]))


def to_column(row):
    n = row.shape[1]
    r, c = (lax.broadcasted_iota(jnp.int32, (n, n), d) for d in (0, 1))
    return jnp.sum(jnp.where(r == c, jnp.broadcast_to(row, (n, n)), 0.0), axis=1, keepdims=True)


def group_partials(total):
    folded = jnp.sum(total.reshape(total.shape[0] // 8, 8, 128), axis=1)
    return jnp.sum(folded, axis=1, keepdims=True)


def stats_row(first, second):
    n = first.shape[0]
    r, c = (lax.broadcasted_iota(jnp.int32, (n, 128), d) for d in (0, 1))
    placed = jnp.where(r == c, first, 0.0) + jnp.where(r + n == c, second, 0.0)
    return jnp.sum(placed, axis=0, keepdims=True)


def stats_columns(row, count, channels):
    groups = channels // GROUP_CHANNELS
    r, c = (lax.broadcasted_iota(jnp.int32, (channels, 128), d) for d in (0, 1))
    wide = jnp.broadcast_to(row, (channels, 128))
    first = jnp.sum(jnp.where(r // GROUP_CHANNELS == c, wide, 0.0), axis=1, keepdims=True)
    second = jnp.sum(
        jnp.where(r // GROUP_CHANNELS + groups == c, wide, 0.0), axis=1, keepdims=True
    )
    mean = first / count
    var = second / count - mean * mean
    return mean, lax.rsqrt(var + EPS)


def gelu(v):
    inner = math.sqrt(2.0 / math.pi) * (v + 0.044715 * (v * v * v))
    return 0.5 * v * (1.0 + jnp.tanh(inner))


TABLES = (
    "fz_hi", "fz_lo", "iz_hi", "iz_lo", "xf_hi", "xf_lo", "xi_hi", "xi_lo",
    "y_tab", "sel_x", "sel_z", "gather", "spread",
)
MSG = 40


class Lazy:
    def __init__(self, refs):
        self.refs = refs

    def __getitem__(self, name):
        return self.refs[name][...]


def lane_roll(a, shift):
    return pltpu.roll(a, shift, axis=1)


def far_first(n):
    return sorted(range(1, n), key=lambda d: -min(d, n - d))


AHEAD = 4


def fused(sizes, *refs):
    wide, narrow, channels = sizes["wide"], sizes["narrow"], sizes["channels"]
    rep = sizes["rep"]
    count = 11 + len(TABLES)
    given, out = refs[:count], refs[count : count + 7]
    scratch = refs[count + 7 :]
    held, loaded, scratch = scratch[:count], scratch[count], scratch[count + 1 :]
    (field, fac_x, fac_y, fac_z, mix, gain, bias, w_in, b_in, w_out, b_out) = held[:11]
    tabs = Lazy(dict(zip(TABLES, held[11:])))
    where_is = {name: 11 + n for n, name in enumerate(TABLES)}
    (
        src, fld, b1, r1, b2, r2, s3, n3, st0, ar1, st1, ar2,
        wts, mix_hi, mix_lo, send, recv, ready,
    ) = scratch
    me_x, me_sp, me_rep = lax.axis_index("sub"), lax.axis_index("sp"), lax.axis_index("rep")
    me_z = me_sp * rep + me_rep
    channel = me_z * narrow + me_x
    chips = wide // rep
    last = (me_sp == 0) & (me_rep == 0)
    turn = jnp.where(last, chips, me_sp)

    def each(low, high, action):
        @pl.loop(low, high)
        def _(position):
            sp = jnp.where(position == chips, 0, position)
            for core in range(rep):

                @pl.when(position > 0 if core == 0 else position < chips)
                def _():
                    action(sp, core)

    def partners(action):
        @pl.when(me_sp > 0)
        def _():
            for core in range(1, rep):
                action(me_sp, (me_rep + core) % rep)

    def z_id(sp, core):
        return {"sp": sp, "rep": core}

    def x_id(s):
        return {"sub": s}

    def x_peer(j):
        s = me_x + j
        return jnp.where(s >= narrow, s - narrow, s)

    def signal(sem, where):
        pl.semaphore_signal(sem, inc=1, device_id=where, device_id_type=pl.DeviceIdType.MESH)

    def push(a, b, slot, where):
        pltpu.make_async_remote_copy(
            src_ref=a, dst_ref=b, send_sem=send.at[slot], recv_sem=recv.at[slot],
            device_id=where, device_id_type=pl.DeviceIdType.MESH,
        ).start()

    def drain(ref, sem):
        pltpu.make_async_copy(ref, ref, sem).wait()

    def rows(start, size):
        return pl.ds(pl.multiple_of(start, 8), size)

    barrier = pltpu.get_barrier_semaphore()

    @pl.loop(1, narrow)
    def _(j):
        signal(barrier, x_id(x_peer(j)))

    partners(lambda sp, core: signal(barrier, z_id(sp, core)))

    loads = [
        pltpu.make_async_copy(a, b, loaded.at[n]) for n, (a, b) in enumerate(zip(given, held))
    ]
    first = [0, where_is["fz_hi"], where_is["fz_lo"], where_is["gather"]]
    later = [n for n in range(count) if n not in first]
    for n in first + later:
        loads[n].start()
    def own_modes(waits):
        for n in waits:
            loads[n].wait()
        parts = [
            jnp.concatenate([field[128 * c + 32 * x : 128 * c + 32 * x + 32] for c in range(8)], 0)
            for x in range(4)
        ]
        main, packed = forward_z(parts, tabs)
        for c in range(8):
            b1[MSG * c : MSG * c + 32] = main[32 * c : 32 * c + 32]
            b1[MSG * c + 32 : MSG * c + 40] = packed[8 * c : 8 * c + 8]

    pl.when(turn == chips)(lambda: own_modes(first))

    before = jnp.where(turn == 0, 0, jnp.where(turn == 1, rep - 1, rep))
    pl.semaphore_wait(barrier, narrow - 1 + (rep - 1) * jnp.minimum(me_sp, 1) + before)

    @pl.when(turn < chips - 1)
    def _():
        for core in range(rep):
            signal(barrier, z_id(turn + 1, core))

    @pl.when(turn == chips - 1)
    def _():
        signal(barrier, z_id(0, 0))

    def send_field(sp, core):
        q = sp * rep + core
        push(src.at[rows(q * 32, 32)], fld.at[rows(me_z * 32, 32)], 1, z_id(sp, core))

    def spread_field():
        for y in range(32):
            src[32 * y : 32 * y + 32] = field[pl.ds(y, 32, stride=32)]
        each(0, turn, send_field)
        partners(send_field)

    def tell_before():
        each(0, turn, lambda sp, core: signal(ready.at[me_z], z_id(sp, core)))

    @pl.when(turn < chips)
    def _():
        tell_before()
        for n in first[:1]:
            loads[n].wait()
        pl.when(turn < chips - 1)(spread_field)
        own_modes(first[1:])

    for j in far_first(narrow):
        s = x_peer(j)
        push(b1.at[rows(s * MSG, MSG)], r1.at[rows(me_x * MSG, MSG)], 0, x_id(s))

    def send_modes(sp, core):
        q = sp * rep + core
        push(s3.at[q], n3.at[me_z], 3, z_id(sp, core))

    pl.when(turn == chips)(tell_before)
    pl.when(turn >= chips - 1)(spread_field)

    r1[rows(me_x * MSG, MSG)] = b1[rows(me_x * MSG, MSG)]
    fld[rows(me_z * 32, 32)] = src[rows(me_z * 32, 32)]
    for n in later:
        loads[n].wait()
    wts[...] = factor_weights(fac_x[...], fac_y[...], fac_z[...], channel, tabs)
    for full, hi, lo in ((mix, mix_hi, mix_lo), (w_in, *out[3:5]), (w_out, *out[5:7])):
        hi[...], lo[...] = split(full[...])
    for n, row in enumerate((gain, bias, b_in, b_out)):
        out[2][n] = jnp.broadcast_to(to_column(row[...]), (channels, 128))

    near = jnp.minimum(turn + 1 + AHEAD, chips + 1)

    def field_when_ready(sp, core):
        pl.semaphore_wait(ready.at[sp * rep + core], 1)
        send_field(sp, core)

    def both_when_ready(sp, core):
        pl.semaphore_wait(ready.at[sp * rep + core], 1)
        send_modes(sp, core)
        send_field(sp, core)

    each(turn + 1, near, field_when_ready)

    drain(r1.at[pl.ds(0, MSG * (narrow - 1))], recv.at[0])
    blocks = [r1[MSG * s : MSG * s + MSG] for s in range(8)]
    main, extra = spectral_filter(blocks, wts[...], tabs, lane_roll)
    for s in range(8):
        b2[MSG * s : MSG * s + 32] = main[s]
        b2[MSG * s + 32 : MSG * s + 40] = extra[s]

    for j in far_first(narrow):
        s = x_peer(j)
        push(b2.at[rows(s * MSG, MSG)], r2.at[rows(me_x * MSG, MSG)], 2, x_id(s))

    r2[rows(me_x * MSG, MSG)] = b2[rows(me_x * MSG, MSG)]
    drain(r2.at[pl.ds(0, MSG * (narrow - 1))], recv.at[2])
    left = leftover_rows([r2[MSG * c + 32 : MSG * c + 40] for c in range(8)], lane_roll)
    for y in range(32):
        s3[y, :8] = r2[pl.ds(y, 8, stride=MSG)]
        s3[y, 8:] = left[y : y + 1]

    @pl.when(near == chips + 1)
    def _():
        for step in far_first(chips):
            sp = me_sp + step
            for core in range(rep):
                send_modes(jnp.where(sp >= chips, sp - chips, sp), core)
        for core in range(1, rep):
            send_modes(me_sp, (me_rep + core) % rep)

    @pl.when(near < chips + 1)
    def _():
        each(0, turn, send_modes)
        partners(send_modes)
        each(turn + 1, near, send_modes)
        each(near, chips + 1, both_when_ready)

    n3[me_z] = s3[me_z]
    drain(n3.at[pl.ds(0, wide - 1)], recv.at[3])
    spectral = inverse_z(
        n3[:, :8].reshape(channels, 128), n3[:, 8:].reshape(wide, 128), (mix_hi[...], mix_lo[...]), tabs
    )
    drain(fld.at[pl.ds(0, 32 * (wide - 1))], recv.at[1])
    first = second = None
    for x in range(4):
        value = spectral[:, 128 * x : 128 * x + 128] + fld[pl.ds(x, channels, stride=4)]
        out[0][x] = value
        first = value if x == 0 else first + value
        second = value * value if x == 0 else second + value * value
    row = stats_row(group_partials(first), group_partials(second))
    st0[0] = row
    ar1[me_z] = row

    for step in far_first(chips):
        sp = me_sp + step
        sp = jnp.where(sp >= chips, sp - chips, sp)
        for core in range(rep):
            push(st0.at[0], ar1.at[me_z], 5, z_id(sp, core))
    for core in range(1, rep):
        push(st0.at[0], ar1.at[me_z], 5, z_id(me_sp, (me_rep + core) % rep))

    drain(ar1.at[pl.ds(0, wide - 1)], recv.at[5])
    row = jnp.sum(ar1[...].reshape(wide, 128), axis=0, keepdims=True)
    st1[0] = row
    ar2[me_x] = row

    for j in far_first(narrow):
        push(st1.at[0], ar2.at[me_x], 6, x_id(x_peer(j)))

    drain(ar2.at[pl.ds(0, narrow - 1)], recv.at[6])
    row = jnp.sum(ar2[...].reshape(narrow, 128), axis=0, keepdims=True)
    out[1][...] = row

    drain(b1.at[pl.ds(0, MSG * (narrow - 1))], send.at[0])
    drain(src.at[pl.ds(0, 32 * (wide - 1))], send.at[1])
    drain(b2.at[pl.ds(0, MSG * (narrow - 1))], send.at[2])
    drain(s3.at[pl.ds(0, wide - 1)], send.at[3])
    drain(ar1.at[pl.ds(0, wide - 1)], send.at[5])
    drain(ar2.at[pl.ds(0, narrow - 1)], send.at[6])


def channel_mlp(count, summed, stats, cols, in_hi, in_lo, out_hi, out_lo, out):
    channels = summed.shape[1]
    mean, inv = stats_columns(stats[...], count, channels)
    mean = jnp.broadcast_to(mean, (channels, 128))
    scale = jnp.broadcast_to(inv, (channels, 128)) * cols[0]
    wide_in, wide_out = (in_hi[...], in_lo[...]), (out_hi[...], out_lo[...])
    for x in range(summed.shape[0]):
        value = summed[x]
        normed = (value - mean) * scale + cols[1]
        hidden = gelu(dot3(wide_in, split(normed)) + cols[2])
        out[pl.ds(x, channels, stride=4)] = value + dot3(wide_out, split(hidden)) + cols[3]


def solution(mesh):
    shape = mesh.shape
    wide, narrow = shape["sp"] * shape["rep"], shape["sub"]
    replicated = P()
    placed = (P(("grp", "sp", "rep"), "sub", None, None),) + (replicated,) * 10

    def local(
        field, mix_weight, factor_x, factor_y, factor_z,
        norm_gain, norm_bias, w_in, b_in, w_out, b_out,
    ):
        held, x_local, ny, nz = field.shape
        channels = mix_weight.shape[0]
        nx = x_local * narrow
        kz = factor_z.shape[1]
        tables = build_tables(nx, ny, nz, kz, held, wide)
        sizes = dict(
            wide=wide, narrow=narrow, channels=channels, rep=shape["rep"],
            count=GROUP_CHANNELS * nx * ny * nz,
        )
        row = lambda v: v.reshape(1, -1)
        operands = [
            field.reshape(held * x_local * ny, nz), factor_x.T, factor_y.T, factor_z.T, mix_weight,
            row(norm_gain), row(norm_bias), w_in, row(b_in), w_out, row(b_out),
        ] + [jnp.asarray(tables[name]) for name in TABLES]
        cells = channels * x_local
        vmem = pl.BlockSpec(memory_space=pltpu.VMEM)
        f32 = lambda *dims: pltpu.VMEM(dims, F32)
        b16 = lambda *dims: pltpu.VMEM(dims, BF16)
        square = (channels, channels)
        handed = pl.pallas_call(
            lambda *refs: fused(sizes, *refs),
            out_shape=(
                jax.ShapeDtypeStruct((x_local, channels, nz), F32),
                jax.ShapeDtypeStruct((1, 128), F32),
                jax.ShapeDtypeStruct((4, channels, 128), F32),
            )
            + (jax.ShapeDtypeStruct(square, BF16),) * 4,
            in_specs=[pl.BlockSpec(memory_space=pltpu.HBM)] * len(operands),
            out_specs=(vmem,) * 7,
            scratch_shapes=[pltpu.VMEM(v.shape, v.dtype) for v in operands]
            + [pltpu.SemaphoreType.DMA((len(operands),))]
            + [
                f32(cells, nz), f32(cells, nz),
                f32(MSG * narrow, 128), f32(MSG * narrow, 128),
                f32(MSG * narrow, 128), f32(MSG * narrow, 128),
                f32(wide, 9, 128), f32(wide, 9, 128),
                f32(1, 1, 128), f32(wide, 1, 128), f32(1, 1, 128), f32(narrow, 1, 128),
                f32(ny, 9 * 128),
                b16(*square), b16(*square),
                pltpu.SemaphoreType.DMA((7,)), pltpu.SemaphoreType.DMA((7,)),
                pltpu.SemaphoreType.REGULAR((wide,)),
            ],
            compiler_params=pltpu.CompilerParams(
                collective_id=0, has_side_effects=True, vmem_limit_bytes=24 * 2**20
            ),
        )(*[pltpu.with_memory_space_constraint(v, pltpu.HBM) for v in operands])
        result = pl.pallas_call(
            functools.partial(channel_mlp, sizes["count"]),
            out_shape=jax.ShapeDtypeStruct((cells, nz), F32),
            in_specs=[vmem] * 7,
            out_specs=vmem,
            compiler_params=pltpu.CompilerParams(vmem_limit_bytes=24 * 2**20),
        )(*handed)
        return result.reshape(channels, x_local, 1, nz)

    return jax.shard_map(
        local,
        mesh=mesh,
        in_specs=placed,
        out_specs=P("grp", "sub", ("sp", "rep"), None),
        check_vma=False,
    )
```

```python
import functools
import math

import jax
import jax.numpy as jnp
import numpy as np
from jax import lax
from jax.experimental import pallas as pl
from jax.experimental.pallas import tpu as pltpu
from jax.sharding import PartitionSpec as P

F32 = jnp.float32
BF16 = jnp.bfloat16
GROUP_CHANNELS = 8
EPS = 1e-05


def split_np(a):
    a = np.asarray(a, np.float32)
    hi = a.astype(BF16)
    lo = (a - hi.astype(np.float32)).astype(BF16)
    return hi, lo


def build_tables(nx, ny, nz, kz, ch_local, wide):
    xl = 4
    chunks = 8
    lane = np.arange(128)
    k_of, x_of, r_of = lane // 16, (lane // 4) % 4, lane % 4
    z = np.arange(nz)
    scale = 1.0 / (nx * ny * nz)
    top = kz // 2
    fwd_z = np.zeros((xl, nz, 256))
    inv_z = np.zeros((256, xl, nz))
    for l in range(128):
        f = 2 * k_of[l] + r_of[l] // 2
        ang = 2 * np.pi * ((f * z) % nz) / nz
        fwd_z[x_of[l], :, l] = (np.cos(ang) if r_of[l] % 2 == 0 else -np.sin(ang)) * scale
        inv_z[l, x_of[l], :] = np.cos(ang) if r_of[l] % 2 == 0 else -np.sin(ang)
        if r_of[l] < 2:
            ang = 2 * np.pi * ((top * z) % nz) / nz
            col = np.cos(ang) if r_of[l] == 0 else -np.sin(ang)
            fwd_z[x_of[l], :, 128 + l] = col * scale
            inv_z[128 + l, x_of[l], :] = col
    fwd_z = fwd_z.reshape(xl * nz, 256)
    inv_z = inv_z.reshape(256, xl * nz)
    ax = np.arange(nx)
    ang = 2 * np.pi * ((ax[:, None] * ax[None, :]) % nx) / nx
    c, s = np.cos(ang), np.sin(ang)
    fwd = np.zeros((nx, 2, 2, nx, 2, 2))
    inv = np.zeros((nx, 2, 2, nx, 2, 2))
    for f in range(2):
        fwd[:, f, 0, :, f, 0] = c
        fwd[:, f, 1, :, f, 0] = s
        fwd[:, f, 0, :, f, 1] = -s
        fwd[:, f, 1, :, f, 1] = c
        inv[:, f, 0, :, f, 0] = c
        inv[:, f, 1, :, f, 0] = -s
        inv[:, f, 0, :, f, 1] = s
        inv[:, f, 1, :, f, 1] = c
    turn = np.zeros((128, 128))
    for l in range(0, 128, 2):
        turn[l + 1, l] = 1.0
        turn[l, l + 1] = -1.0
    fwd = fwd.reshape(128, 128)
    inv = inv.reshape(128, 128)
    x_fwd = np.concatenate([fwd, fwd @ turn], 1)
    x_inv = np.concatenate([inv, -(inv @ turn)], 1)
    ay = np.arange(ny)
    ang = 2 * np.pi * ((ay[:, None] * ay[None, :]) % ny) / ny
    y_tab = np.concatenate([np.cos(ang), np.sin(ang)], 1)
    hi, lo = split_np(y_tab)
    y_tab3 = np.concatenate([hi, hi, lo], 1)
    sel_x = np.zeros((nx, 256))
    for a in range(nx):
        sel_x[a, 4 * a : 4 * a + 4] = 1.0
        sel_x[a, 128 + 4 * ((nx - a) % nx) : 128 + 4 * ((nx - a) % nx) + 4] = 1.0
    sel_z = np.zeros((kz, 2, 9, nx, 4))
    for f in range(top + 1):
        k, f2 = f // 2, f % 2
        if f < top:
            sel_z[f, 0, k, :, 2 * f2 : 2 * f2 + 2] = 1.0
        if f > 0:
            sel_z[kz - f, 1, k, :, 2 * f2 : 2 * f2 + 2] = 1.0
    sel_z = sel_z.reshape(kz, 2 * 9 * 128)
    rows_in = np.arange(ch_local * ny)
    rows_out = np.arange(ch_local * 8)
    gather = (
        (rows_in[None, :] // ny == rows_out[:, None] // 8)
        & (rows_in[None, :] % 8 == rows_out[:, None] % 8)
    ).astype(np.float32)
    rows_all = np.arange(ch_local * wide)
    spread = (rows_all[:, None] // ch_local == np.arange(wide)[None, :]).astype(np.float32)
    fz = split_np(fwd_z)
    iz = split_np(inv_z)
    xf = split_np(x_fwd)
    xi = split_np(x_inv)
    return dict(
        fz_hi=fz[0], fz_lo=fz[1], iz_hi=iz[0], iz_lo=iz[1],
        xf_hi=xf[0], xf_lo=xf[1], xi_hi=xi[0], xi_lo=xi[1],
        y_tab=y_tab3,
        sel_x=sel_x.astype(np.float32), sel_z=sel_z.astype(np.float32),
        gather=gather.astype(BF16), spread=spread.astype(BF16),
    )


def split(a):
    hi = a.astype(BF16)
    return hi, (a - hi.astype(F32)).astype(BF16)


def dot1(a, b):
    return lax.dot_general(a, b, (((1,), (0,)), ((), ())), preferred_element_type=F32)


def dot3(a, b):
    return dot1(a[0], b[0]) + dot1(a[0], b[1]) + dot1(a[1], b[0])


def swap_chunks(arrays, roll):
    arrays = list(arrays)
    rows = arrays[0].shape[0]
    chunk = lax.broadcasted_iota(jnp.int32, (rows, 128), 1) // 16
    for d in (4, 2, 1):
        upper = (chunk // d) % 2 == 1
        for i in range(8):
            if (i // d) % 2 == 0:
                low, high = arrays[i], arrays[i + d]
                arrays[i] = jnp.where(upper, roll(high, 16 * d), low)
                arrays[i + d] = jnp.where(upper, high, roll(low, 128 - 16 * d))
    return arrays


def forward_z(parts, tabs):
    fz_hi, fz_lo = tabs["fz_hi"], tabs["fz_lo"]
    total = None
    for x, part in enumerate(parts):
        term = dot3(split(part), (fz_hi[128 * x : 128 * x + 128], fz_lo[128 * x : 128 * x + 128]))
        total = term if total is None else total + term
    main, extra = total[:, :128], total[:, 128:]
    rows, lanes = (lax.broadcasted_iota(jnp.int32, extra.shape, d) for d in (0, 1))
    extra = jnp.where((rows % 32) // 8 == lanes // 16, extra, 0.0)
    hi, lo = split(extra)
    packed = dot1(tabs["gather"], hi) + dot1(tabs["gather"], lo)
    return main, packed


def factor_weights(fac_x, fac_y, fac_z, channel, tabs):
    n, channels = fac_y.shape
    own = lax.broadcasted_iota(jnp.int32, (n, channels), 1) == channel
    col_x, col_y, col_z = (
        jnp.sum(jnp.where(own, f, 0.0), axis=1, keepdims=True) for f in (fac_x, fac_y, fac_z)
    )
    lanes_x = jnp.sum(col_x * tabs["sel_x"], axis=0, keepdims=True)
    lanes_z = jnp.sum(col_z * tabs["sel_z"], axis=0, keepdims=True)
    plus = lanes_z[:, :1152] * jnp.concatenate([lanes_x[:, :128]] * 9, 1)
    minus = lanes_z[:, 1152:] * jnp.concatenate([lanes_x[:, 128:]] * 9, 1)
    r, c = (lax.broadcasted_iota(jnp.int32, (n, n), d) for d in (0, 1))
    row_y = jnp.sum(jnp.where(r == c, col_y, 0.0), axis=0, keepdims=True)
    flipped = jnp.where((n - r) % n == c, jnp.broadcast_to(row_y, (n, n)), 0.0)
    col_minus = jnp.sum(flipped, axis=1, keepdims=True)
    return col_y * plus + col_minus * minus


def spectral_filter(blocks, weights, tabs, roll):
    main = swap_chunks([b[:32] for b in blocks], roll)
    extra = swap_chunks([b[32:40] for b in blocks], roll)
    last = jnp.concatenate(extra[:4], 0)
    rows = jnp.concatenate(main + [last], 0)

    def along_y(pairs):
        stacked = jnp.concatenate(
            [
                jnp.concatenate(
                    [pairs[32 * k : 32 * k + 32, :128], pairs[32 * k : 32 * k + 32, 128:]], 0
                )
                for k in range(9)
            ],
            1,
        )
        hi, lo = split(stacked)
        return dot1(tabs["y_tab"], jnp.concatenate([hi, lo, hi], 0))

    pairs = dot3(split(rows), (tabs["xf_hi"], tabs["xf_lo"]))
    spec = along_y(pairs) * weights
    rows = jnp.concatenate([spec[:, 128 * k : 128 * k + 128] for k in range(9)], 0)
    pairs = dot3(split(rows), (tabs["xi_hi"], tabs["xi_lo"]))
    back = along_y(pairs)
    main = swap_chunks([back[:, 128 * k : 128 * k + 128] for k in range(8)], roll)
    last = back[:, 1024:]
    tiles = [last[8 * p : 8 * p + 8] for p in range(4)] + [jnp.zeros((8, 128), F32)] * 4
    extra = swap_chunks(tiles, roll)
    return main, extra


def leftover_rows(extras, roll):
    return jnp.concatenate(swap_chunks(extras, roll)[:4], 0)


def inverse_z(modes, left, mix, tabs):
    hi, lo = split(left)
    wide = dot1(tabs["spread"], hi) + dot1(tabs["spread"], lo)
    rows, lanes = (lax.broadcasted_iota(jnp.int32, wide.shape, d) for d in (0, 1))
    wide = jnp.where(rows % 8 == lanes // 16, wide, 0.0)
    both = jnp.concatenate([modes, wide], 1)
    mixed = dot3(mix, split(both))
    return dot3(split(mixed), (tabs["iz_hi"], tabs["iz_lo"]))


def to_column(row):
    n = row.shape[1]
    r, c = (lax.broadcasted_iota(jnp.int32, (n, n), d) for d in (0, 1))
    return jnp.sum(jnp.where(r == c, jnp.broadcast_to(row, (n, n)), 0.0), axis=1, keepdims=True)


def group_partials(total):
    folded = jnp.sum(total.reshape(total.shape[0] // 8, 8, 128), axis=1)
    return jnp.sum(folded, axis=1, keepdims=True)


def stats_row(first, second):
    n = first.shape[0]
    r, c = (lax.broadcasted_iota(jnp.int32, (n, 128), d) for d in (0, 1))
    placed = jnp.where(r == c, first, 0.0) + jnp.where(r + n == c, second, 0.0)
    return jnp.sum(placed, axis=0, keepdims=True)


def stats_columns(row, count, channels):
    groups = channels // GROUP_CHANNELS
    r, c = (lax.broadcasted_iota(jnp.int32, (channels, 128), d) for d in (0, 1))
    wide = jnp.broadcast_to(row, (channels, 128))
    first = jnp.sum(jnp.where(r // GROUP_CHANNELS == c, wide, 0.0), axis=1, keepdims=True)
    second = jnp.sum(
        jnp.where(r // GROUP_CHANNELS + groups == c, wide, 0.0), axis=1, keepdims=True
    )
    mean = first / count
    var = second / count - mean * mean
    return mean, lax.rsqrt(var + EPS)


def gelu(v):
    inner = math.sqrt(2.0 / math.pi) * (v + 0.044715 * (v * v * v))
    return 0.5 * v * (1.0 + jnp.tanh(inner))


TABLES = (
    "fz_hi", "fz_lo", "iz_hi", "iz_lo", "xf_hi", "xf_lo", "xi_hi", "xi_lo",
    "y_tab", "sel_x", "sel_z", "gather", "spread",
)
MSG = 36


class Lazy:
    def __init__(self, refs):
        self.refs = refs

    def __getitem__(self, name):
        return self.refs[name][...]


def lane_roll(a, shift):
    return pltpu.roll(a, shift, axis=1)


def fold(tile):
    return tile[:4] + lane_roll(tile[4:], 64)


def unfold(tile):
    return jnp.concatenate([tile, lane_roll(tile, 64)], 0)


def far_first(n):
    return sorted(range(1, n), key=lambda d: -min(d, n - d))


AHEAD = 4


def fused(sizes, *refs):
    wide, narrow, channels = sizes["wide"], sizes["narrow"], sizes["channels"]
    rep = sizes["rep"]
    count = 11 + len(TABLES)
    given, out = refs[:count], refs[count : count + 7]
    scratch = refs[count + 7 :]
    held, loaded, scratch = scratch[:count], scratch[count], scratch[count + 1 :]
    (field, fac_x, fac_y, fac_z, mix, gain, bias, w_in, b_in, w_out, b_out) = held[:11]
    tabs = Lazy(dict(zip(TABLES, held[11:])))
    where_is = {name: 11 + n for n, name in enumerate(TABLES)}
    (
        src, fld, b1, r1, b2, r2, s3, n3, st0, ar1, st1, ar2,
        wts, mix_hi, mix_lo, send, recv, ready,
    ) = scratch
    me_x, me_sp, me_rep = lax.axis_index("sub"), lax.axis_index("sp"), lax.axis_index("rep")
    me_z = me_sp * rep + me_rep
    channel = me_z * narrow + me_x
    chips = wide // rep
    last = (me_sp == 0) & (me_rep == 0)
    turn = jnp.where(last, chips, me_sp)

    def each(low, high, action):
        @pl.loop(low, high)
        def _(position):
            sp = jnp.where(position == chips, 0, position)
            for core in range(rep):

                @pl.when(position > 0 if core == 0 else position < chips)
                def _():
                    action(sp, core)

    def partners(action):
        @pl.when(me_sp > 0)
        def _():
            for core in range(1, rep):
                action(me_sp, (me_rep + core) % rep)

    def z_id(sp, core):
        return {"sp": sp, "rep": core}

    def x_id(s):
        return {"sub": s}

    def x_peer(j):
        s = me_x + j
        return jnp.where(s >= narrow, s - narrow, s)

    def signal(sem, where):
        pl.semaphore_signal(sem, inc=1, device_id=where, device_id_type=pl.DeviceIdType.MESH)

    def push(a, b, slot, where):
        pltpu.make_async_remote_copy(
            src_ref=a, dst_ref=b, send_sem=send.at[slot], recv_sem=recv.at[slot],
            device_id=where, device_id_type=pl.DeviceIdType.MESH,
        ).start()

    def drain(ref, sem):
        pltpu.make_async_copy(ref, ref, sem).wait()

    def rows(start, size):
        return pl.ds(pl.multiple_of(start, 8), size)

    barrier = pltpu.get_barrier_semaphore()

    @pl.loop(1, narrow)
    def _(j):
        signal(barrier, x_id(x_peer(j)))

    partners(lambda sp, core: signal(barrier, z_id(sp, core)))

    loads = [
        pltpu.make_async_copy(a, b, loaded.at[n]) for n, (a, b) in enumerate(zip(given, held))
    ]
    first = [0, where_is["fz_hi"], where_is["fz_lo"], where_is["gather"]]
    later = [n for n in range(count) if n not in first]
    for n in first + later:
        loads[n].start()
    def own_modes(waits):
        for n in waits:
            loads[n].wait()
        parts = [
            jnp.concatenate([field[128 * c + 32 * x : 128 * c + 32 * x + 32] for c in range(8)], 0)
            for x in range(4)
        ]
        main, packed = forward_z(parts, tabs)
        for c in range(8):
            b1[c, :32] = main[32 * c : 32 * c + 32]
            b1[c, 32:] = fold(packed[8 * c : 8 * c + 8])

    pl.when(turn == chips)(lambda: own_modes(first))

    before = jnp.where(turn == 0, 0, jnp.where(turn == 1, rep - 1, rep))
    pl.semaphore_wait(barrier, narrow - 1 + (rep - 1) * jnp.minimum(me_sp, 1) + before)

    @pl.when(turn < chips - 1)
    def _():
        for core in range(rep):
            signal(barrier, z_id(turn + 1, core))

    @pl.when(turn == chips - 1)
    def _():
        signal(barrier, z_id(0, 0))

    def send_field(sp, core):
        q = sp * rep + core
        push(src.at[rows(q * 32, 32)], fld.at[rows(me_z * 32, 32)], 1, z_id(sp, core))

    def spread_field():
        for y in range(32):
            src[32 * y : 32 * y + 32] = field[pl.ds(y, 32, stride=32)]
        each(0, turn, send_field)
        partners(send_field)

    def tell_before():
        each(0, turn, lambda sp, core: signal(ready.at[me_z], z_id(sp, core)))

    @pl.when(turn < chips)
    def _():
        tell_before()
        for n in first[:1]:
            loads[n].wait()
        pl.when(turn < chips - 1)(spread_field)
        own_modes(first[1:])

    for j in far_first(narrow):
        s = x_peer(j)
        push(b1.at[s], r1.at[me_x], 0, x_id(s))

    def send_modes(sp, core):
        q = sp * rep + core
        push(s3.at[q], n3.at[me_z], 3, z_id(sp, core))

    pl.when(turn == chips)(tell_before)
    pl.when(turn >= chips - 1)(spread_field)

    r1[me_x] = b1[me_x]
    fld[rows(me_z * 32, 32)] = src[rows(me_z * 32, 32)]
    for n in later:
        loads[n].wait()
    wts[...] = factor_weights(fac_x[...], fac_y[...], fac_z[...], channel, tabs)
    for full, hi, lo in ((mix, mix_hi, mix_lo), (w_in, *out[3:5]), (w_out, *out[5:7])):
        hi[...], lo[...] = split(full[...])
    for n, row in enumerate((gain, bias, b_in, b_out)):
        out[2][n] = jnp.broadcast_to(to_column(row[...]), (channels, 128))

    near = jnp.minimum(turn + 1 + AHEAD, chips + 1)

    def field_when_ready(sp, core):
        pl.semaphore_wait(ready.at[sp * rep + core], 1)
        send_field(sp, core)

    def both_when_ready(sp, core):
        pl.semaphore_wait(ready.at[sp * rep + core], 1)
        send_modes(sp, core)
        send_field(sp, core)

    each(turn + 1, near, field_when_ready)

    drain(r1.at[pl.ds(0, narrow - 1)], recv.at[0])
    blocks = [jnp.concatenate([r1[s, :32], unfold(r1[s, 32:])], 0) for s in range(8)]
    main, extra = spectral_filter(blocks, wts[...], tabs, lane_roll)
    for s in range(8):
        b2[s, :32] = main[s]
        b2[s, 32:] = fold(extra[s])

    for j in far_first(narrow):
        s = x_peer(j)
        push(b2.at[s], r2.at[me_x], 2, x_id(s))

    r2[me_x] = b2[me_x]
    drain(r2.at[pl.ds(0, narrow - 1)], recv.at[2])
    left = leftover_rows([unfold(r2[c, 32:]) for c in range(8)], lane_roll)
    for y in range(32):
        s3[y, :8] = r2[:, y]
        s3[y, 8:] = left[y : y + 1]

    @pl.when(near == chips + 1)
    def _():
        for step in far_first(chips):
            sp = me_sp + step
            for core in range(rep):
                send_modes(jnp.where(sp >= chips, sp - chips, sp), core)
        for core in range(1, rep):
            send_modes(me_sp, (me_rep + core) % rep)

    @pl.when(near < chips + 1)
    def _():
        each(0, turn, send_modes)
        partners(send_modes)
        each(turn + 1, near, send_modes)
        each(near, chips + 1, both_when_ready)

    n3[me_z] = s3[me_z]
    drain(n3.at[pl.ds(0, wide - 1)], recv.at[3])
    spectral = inverse_z(
        n3[:, :8].reshape(channels, 128), n3[:, 8:].reshape(wide, 128), (mix_hi[...], mix_lo[...]), tabs
    )
    drain(fld.at[pl.ds(0, 32 * (wide - 1))], recv.at[1])
    first = second = None
    for x in range(4):
        value = spectral[:, 128 * x : 128 * x + 128] + fld[pl.ds(x, channels, stride=4)]
        out[0][x] = value
        first = value if x == 0 else first + value
        second = value * value if x == 0 else second + value * value
    row = stats_row(group_partials(first), group_partials(second))
    st0[0] = row
    ar1[me_z] = row

    for step in far_first(chips):
        sp = me_sp + step
        sp = jnp.where(sp >= chips, sp - chips, sp)
        for core in range(rep):
            push(st0.at[0], ar1.at[me_z], 5, z_id(sp, core))
    for core in range(1, rep):
        push(st0.at[0], ar1.at[me_z], 5, z_id(me_sp, (me_rep + core) % rep))

    drain(ar1.at[pl.ds(0, wide - 1)], recv.at[5])
    row = jnp.sum(ar1[...].reshape(wide, 128), axis=0, keepdims=True)
    st1[0] = row
    ar2[me_x] = row

    for j in far_first(narrow):
        push(st1.at[0], ar2.at[me_x], 6, x_id(x_peer(j)))

    drain(ar2.at[pl.ds(0, narrow - 1)], recv.at[6])
    row = jnp.sum(ar2[...].reshape(narrow, 128), axis=0, keepdims=True)
    out[1][...] = row

    drain(b1.at[pl.ds(0, narrow - 1)], send.at[0])
    drain(src.at[pl.ds(0, 32 * (wide - 1))], send.at[1])
    drain(b2.at[pl.ds(0, narrow - 1)], send.at[2])
    drain(s3.at[pl.ds(0, wide - 1)], send.at[3])
    drain(ar1.at[pl.ds(0, wide - 1)], send.at[5])
    drain(ar2.at[pl.ds(0, narrow - 1)], send.at[6])


def channel_mlp(count, summed, stats, cols, in_hi, in_lo, out_hi, out_lo, out):
    channels = summed.shape[1]
    mean, inv = stats_columns(stats[...], count, channels)
    mean = jnp.broadcast_to(mean, (channels, 128))
    scale = jnp.broadcast_to(inv, (channels, 128)) * cols[0]
    wide_in, wide_out = (in_hi[...], in_lo[...]), (out_hi[...], out_lo[...])
    for x in range(summed.shape[0]):
        value = summed[x]
        normed = (value - mean) * scale + cols[1]
        hidden = gelu(dot3(wide_in, split(normed)) + cols[2])
        out[pl.ds(x, channels, stride=4)] = value + dot3(wide_out, split(hidden)) + cols[3]


def solution(mesh):
    shape = mesh.shape
    wide, narrow = shape["sp"] * shape["rep"], shape["sub"]
    replicated = P()
    placed = (P(("grp", "sp", "rep"), "sub", None, None),) + (replicated,) * 10

    def local(
        field, mix_weight, factor_x, factor_y, factor_z,
        norm_gain, norm_bias, w_in, b_in, w_out, b_out,
    ):
        held, x_local, ny, nz = field.shape
        channels = mix_weight.shape[0]
        nx = x_local * narrow
        kz = factor_z.shape[1]
        tables = build_tables(nx, ny, nz, kz, held, wide)
        sizes = dict(
            wide=wide, narrow=narrow, channels=channels, rep=shape["rep"],
            count=GROUP_CHANNELS * nx * ny * nz,
        )
        row = lambda v: v.reshape(1, -1)
        operands = [
            field.reshape(held * x_local * ny, nz), factor_x.T, factor_y.T, factor_z.T, mix_weight,
            row(norm_gain), row(norm_bias), w_in, row(b_in), w_out, row(b_out),
        ] + [jnp.asarray(tables[name]) for name in TABLES]
        cells = channels * x_local
        vmem = pl.BlockSpec(memory_space=pltpu.VMEM)
        f32 = lambda *dims: pltpu.VMEM(dims, F32)
        b16 = lambda *dims: pltpu.VMEM(dims, BF16)
        square = (channels, channels)
        handed = pl.pallas_call(
            lambda *refs: fused(sizes, *refs),
            out_shape=(
                jax.ShapeDtypeStruct((x_local, channels, nz), F32),
                jax.ShapeDtypeStruct((1, 128), F32),
                jax.ShapeDtypeStruct((4, channels, 128), F32),
            )
            + (jax.ShapeDtypeStruct(square, BF16),) * 4,
            in_specs=[pl.BlockSpec(memory_space=pltpu.HBM)] * len(operands),
            out_specs=(vmem,) * 7,
            scratch_shapes=[pltpu.VMEM(v.shape, v.dtype) for v in operands]
            + [pltpu.SemaphoreType.DMA((len(operands),))]
            + [
                f32(cells, nz), f32(cells, nz),
                f32(narrow, MSG, 128), f32(narrow, MSG, 128),
                f32(narrow, MSG, 128), f32(narrow, MSG, 128),
                f32(wide, 9, 128), f32(wide, 9, 128),
                f32(1, 1, 128), f32(wide, 1, 128), f32(1, 1, 128), f32(narrow, 1, 128),
                f32(ny, 9 * 128),
                b16(*square), b16(*square),
                pltpu.SemaphoreType.DMA((7,)), pltpu.SemaphoreType.DMA((7,)),
                pltpu.SemaphoreType.REGULAR((wide,)),
            ],
            compiler_params=pltpu.CompilerParams(
                collective_id=0, has_side_effects=True, vmem_limit_bytes=24 * 2**20
            ),
        )(*[pltpu.with_memory_space_constraint(v, pltpu.HBM) for v in operands])
        result = pl.pallas_call(
            functools.partial(channel_mlp, sizes["count"]),
            out_shape=jax.ShapeDtypeStruct((cells, nz), F32),
            in_specs=[vmem] * 7,
            out_specs=vmem,
            compiler_params=pltpu.CompilerParams(vmem_limit_bytes=24 * 2**20),
        )(*handed)
        return result.reshape(channels, x_local, 1, nz)

    return jax.shard_map(
        local,
        mesh=mesh,
        in_specs=placed,
        out_specs=P("grp", "sub", ("sp", "rep"), None),
        check_vma=False,
    )
```

```python
import functools
import math

import jax
import jax.numpy as jnp
import numpy as np
from jax import lax
from jax.experimental import pallas as pl
from jax.experimental.pallas import tpu as pltpu
from jax.sharding import PartitionSpec as P

F32 = jnp.float32
BF16 = jnp.bfloat16
GROUP_CHANNELS = 8
EPS = 1e-05


def split_np(a):
    a = np.asarray(a, np.float32)
    hi = a.astype(BF16)
    lo = (a - hi.astype(np.float32)).astype(BF16)
    return hi, lo


def build_tables(nx, ny, nz, kz, ch_local, wide):
    xl = 4
    chunks = 8
    lane = np.arange(128)
    k_of, x_of, r_of = lane // 16, (lane // 4) % 4, lane % 4
    z = np.arange(nz)
    scale = 1.0 / (nx * ny * nz)
    top = kz // 2
    fwd_z = np.zeros((xl, nz, 256))
    inv_z = np.zeros((256, xl, nz))
    for l in range(128):
        f = 2 * k_of[l] + r_of[l] // 2
        ang = 2 * np.pi * ((f * z) % nz) / nz
        fwd_z[x_of[l], :, l] = (np.cos(ang) if r_of[l] % 2 == 0 else -np.sin(ang)) * scale
        inv_z[l, x_of[l], :] = np.cos(ang) if r_of[l] % 2 == 0 else -np.sin(ang)
        if r_of[l] < 2:
            ang = 2 * np.pi * ((top * z) % nz) / nz
            col = np.cos(ang) if r_of[l] == 0 else -np.sin(ang)
            fwd_z[x_of[l], :, 128 + l] = col * scale
            inv_z[128 + l, x_of[l], :] = col
    fwd_z = fwd_z.reshape(xl * nz, 256)
    inv_z = inv_z.reshape(256, xl * nz)
    ax = np.arange(nx)
    ang = 2 * np.pi * ((ax[:, None] * ax[None, :]) % nx) / nx
    c, s = np.cos(ang), np.sin(ang)
    fwd = np.zeros((nx, 2, 2, nx, 2, 2))
    inv = np.zeros((nx, 2, 2, nx, 2, 2))
    for f in range(2):
        fwd[:, f, 0, :, f, 0] = c
        fwd[:, f, 1, :, f, 0] = s
        fwd[:, f, 0, :, f, 1] = -s
        fwd[:, f, 1, :, f, 1] = c
        inv[:, f, 0, :, f, 0] = c
        inv[:, f, 1, :, f, 0] = -s
        inv[:, f, 0, :, f, 1] = s
        inv[:, f, 1, :, f, 1] = c
    turn = np.zeros((128, 128))
    for l in range(0, 128, 2):
        turn[l + 1, l] = 1.0
        turn[l, l + 1] = -1.0
    fwd = fwd.reshape(128, 128)
    inv = inv.reshape(128, 128)
    x_fwd = np.concatenate([fwd, fwd @ turn], 1)
    x_inv = np.concatenate([inv, -(inv @ turn)], 1)
    ay = np.arange(ny)
    ang = 2 * np.pi * ((ay[:, None] * ay[None, :]) % ny) / ny
    y_tab = np.concatenate([np.cos(ang), np.sin(ang)], 1)
    hi, lo = split_np(y_tab)
    y_tab3 = np.concatenate([hi, hi, lo], 1)
    sel_x = np.zeros((nx, 256))
    for a in range(nx):
        sel_x[a, 4 * a : 4 * a + 4] = 1.0
        sel_x[a, 128 + 4 * ((nx - a) % nx) : 128 + 4 * ((nx - a) % nx) + 4] = 1.0
    sel_z = np.zeros((kz, 2, 9, nx, 4))
    for f in range(top + 1):
        k, f2 = f // 2, f % 2
        if f < top:
            sel_z[f, 0, k, :, 2 * f2 : 2 * f2 + 2] = 1.0
        if f > 0:
            sel_z[kz - f, 1, k, :, 2 * f2 : 2 * f2 + 2] = 1.0
    sel_z = sel_z.reshape(kz, 2 * 9 * 128)
    rows_in = np.arange(ch_local * ny)
    rows_out = np.arange(ch_local * 8)
    gather = (
        (rows_in[None, :] // ny == rows_out[:, None] // 8)
        & (rows_in[None, :] % 8 == rows_out[:, None] % 8)
    ).astype(np.float32)
    rows_all = np.arange(ch_local * wide)
    spread = (rows_all[:, None] // ch_local == np.arange(wide)[None, :]).astype(np.float32)
    fz = split_np(fwd_z)
    iz = split_np(inv_z)
    xf = split_np(x_fwd)
    xi = split_np(x_inv)
    return dict(
        fz_hi=fz[0], fz_lo=fz[1], iz_hi=iz[0], iz_lo=iz[1],
        xf_hi=xf[0], xf_lo=xf[1], xi_hi=xi[0], xi_lo=xi[1],
        y_tab=y_tab3,
        sel_x=sel_x.astype(np.float32), sel_z=sel_z.astype(np.float32),
        gather=gather.astype(BF16), spread=spread.astype(BF16),
    )


def split(a):
    hi = a.astype(BF16)
    return hi, (a - hi.astype(F32)).astype(BF16)


def dot1(a, b):
    return lax.dot_general(a, b, (((1,), (0,)), ((), ())), preferred_element_type=F32)


def dot3(a, b):
    return dot1(a[0], b[0]) + dot1(a[0], b[1]) + dot1(a[1], b[0])


def swap_chunks(arrays, roll):
    arrays = list(arrays)
    rows = arrays[0].shape[0]
    chunk = lax.broadcasted_iota(jnp.int32, (rows, 128), 1) // 16
    for d in (4, 2, 1):
        upper = (chunk // d) % 2 == 1
        for i in range(8):
            if (i // d) % 2 == 0:
                low, high = arrays[i], arrays[i + d]
                arrays[i] = jnp.where(upper, roll(high, 16 * d), low)
                arrays[i + d] = jnp.where(upper, high, roll(low, 128 - 16 * d))
    return arrays


def forward_z(parts, tabs):
    fz_hi, fz_lo = tabs["fz_hi"], tabs["fz_lo"]
    total = None
    for x, part in enumerate(parts):
        term = dot3(split(part), (fz_hi[128 * x : 128 * x + 128], fz_lo[128 * x : 128 * x + 128]))
        total = term if total is None else total + term
    main, extra = total[:, :128], total[:, 128:]
    rows, lanes = (lax.broadcasted_iota(jnp.int32, extra.shape, d) for d in (0, 1))
    extra = jnp.where((rows % 32) // 8 == lanes // 16, extra, 0.0)
    hi, lo = split(extra)
    packed = dot1(tabs["gather"], hi) + dot1(tabs["gather"], lo)
    return main, packed


def factor_weights(fac_x, fac_y, fac_z, channel, tabs):
    n, channels = fac_y.shape
    own = lax.broadcasted_iota(jnp.int32, (n, channels), 1) == channel
    col_x, col_y, col_z = (
        jnp.sum(jnp.where(own, f, 0.0), axis=1, keepdims=True) for f in (fac_x, fac_y, fac_z)
    )
    lanes_x = jnp.sum(col_x * tabs["sel_x"], axis=0, keepdims=True)
    lanes_z = jnp.sum(col_z * tabs["sel_z"], axis=0, keepdims=True)
    plus = lanes_z[:, :1152] * jnp.concatenate([lanes_x[:, :128]] * 9, 1)
    minus = lanes_z[:, 1152:] * jnp.concatenate([lanes_x[:, 128:]] * 9, 1)
    r, c = (lax.broadcasted_iota(jnp.int32, (n, n), d) for d in (0, 1))
    row_y = jnp.sum(jnp.where(r == c, col_y, 0.0), axis=0, keepdims=True)
    flipped = jnp.where((n - r) % n == c, jnp.broadcast_to(row_y, (n, n)), 0.0)
    col_minus = jnp.sum(flipped, axis=1, keepdims=True)
    return col_y * plus + col_minus * minus


def spectral_filter(blocks, weights, tabs, roll):
    main = swap_chunks([b[:32] for b in blocks], roll)
    extra = swap_chunks([b[32:40] for b in blocks], roll)
    last = jnp.concatenate(extra[:4], 0)
    rows = jnp.concatenate(main + [last], 0)

    def along_y(pairs):
        stacked = jnp.concatenate(
            [
                jnp.concatenate(
                    [pairs[32 * k : 32 * k + 32, :128], pairs[32 * k : 32 * k + 32, 128:]], 0
                )
                for k in range(9)
            ],
            1,
        )
        hi, lo = split(stacked)
        return dot1(tabs["y_tab"], jnp.concatenate([hi, lo, hi], 0))

    pairs = dot3(split(rows), (tabs["xf_hi"], tabs["xf_lo"]))
    spec = along_y(pairs) * weights
    rows = jnp.concatenate([spec[:, 128 * k : 128 * k + 128] for k in range(9)], 0)
    pairs = dot3(split(rows), (tabs["xi_hi"], tabs["xi_lo"]))
    back = along_y(pairs)
    main = swap_chunks([back[:, 128 * k : 128 * k + 128] for k in range(8)], roll)
    last = back[:, 1024:]
    tiles = [last[8 * p : 8 * p + 8] for p in range(4)] + [jnp.zeros((8, 128), F32)] * 4
    extra = swap_chunks(tiles, roll)
    return main, extra


def leftover_rows(extras, roll):
    return jnp.concatenate(swap_chunks(extras, roll)[:4], 0)


def inverse_z(modes, left, mix, tabs):
    hi, lo = split(left)
    wide = dot1(tabs["spread"], hi) + dot1(tabs["spread"], lo)
    rows, lanes = (lax.broadcasted_iota(jnp.int32, wide.shape, d) for d in (0, 1))
    wide = jnp.where(rows % 8 == lanes // 16, wide, 0.0)
    both = jnp.concatenate([modes, wide], 1)
    mixed = dot3(mix, split(both))
    return dot3(split(mixed), (tabs["iz_hi"], tabs["iz_lo"]))


def to_column(row):
    n = row.shape[1]
    r, c = (lax.broadcasted_iota(jnp.int32, (n, n), d) for d in (0, 1))
    return jnp.sum(jnp.where(r == c, jnp.broadcast_to(row, (n, n)), 0.0), axis=1, keepdims=True)


def group_partials(total):
    folded = jnp.sum(total.reshape(total.shape[0] // 8, 8, 128), axis=1)
    return jnp.sum(folded, axis=1, keepdims=True)


def stats_row(first, second):
    n = first.shape[0]
    r, c = (lax.broadcasted_iota(jnp.int32, (n, 128), d) for d in (0, 1))
    placed = jnp.where(r == c, first, 0.0) + jnp.where(r + n == c, second, 0.0)
    return jnp.sum(placed, axis=0, keepdims=True)


def stats_columns(row, count, channels):
    groups = channels // GROUP_CHANNELS
    r, c = (lax.broadcasted_iota(jnp.int32, (channels, 128), d) for d in (0, 1))
    wide = jnp.broadcast_to(row, (channels, 128))
    first = jnp.sum(jnp.where(r // GROUP_CHANNELS == c, wide, 0.0), axis=1, keepdims=True)
    second = jnp.sum(
        jnp.where(r // GROUP_CHANNELS + groups == c, wide, 0.0), axis=1, keepdims=True
    )
    mean = first / count
    var = second / count - mean * mean
    return mean, lax.rsqrt(var + EPS)


def gelu(v):
    inner = math.sqrt(2.0 / math.pi) * (v + 0.044715 * (v * v * v))
    return 0.5 * v * (1.0 + jnp.tanh(inner))


TABLES = (
    "fz_hi", "fz_lo", "iz_hi", "iz_lo", "xf_hi", "xf_lo", "xi_hi", "xi_lo",
    "y_tab", "sel_x", "sel_z", "gather", "spread",
)
MSG = 36


class Lazy:
    def __init__(self, refs):
        self.refs = refs

    def __getitem__(self, name):
        return self.refs[name][...]


def lane_roll(a, shift):
    return pltpu.roll(a, shift, axis=1)


def fold(tile):
    return tile[:4] + lane_roll(tile[4:], 64)


def unfold(tile):
    return jnp.concatenate([tile, lane_roll(tile, 64)], 0)


def far_first(n):
    return sorted(range(1, n), key=lambda d: -min(d, n - d))


AHEAD = 5


def fused(sizes, *refs):
    wide, narrow, channels = sizes["wide"], sizes["narrow"], sizes["channels"]
    rep = sizes["rep"]
    count = 11 + len(TABLES)
    given, out = refs[:count], refs[count : count + 7]
    scratch = refs[count + 7 :]
    held, loaded, scratch = scratch[:count], scratch[count], scratch[count + 1 :]
    (field, fac_x, fac_y, fac_z, mix, gain, bias, w_in, b_in, w_out, b_out) = held[:11]
    tabs = Lazy(dict(zip(TABLES, held[11:])))
    where_is = {name: 11 + n for n, name in enumerate(TABLES)}
    (
        src, fld, b1, r1, b2, r2, s3, n3, st0, ar1, st1, ar2,
        wts, mix_hi, mix_lo, send, recv, ready,
    ) = scratch
    me_x, me_sp, me_rep = lax.axis_index("sub"), lax.axis_index("sp"), lax.axis_index("rep")
    me_z = me_sp * rep + me_rep
    channel = me_z * narrow + me_x
    chips = wide // rep
    last = (me_sp == 0) & (me_rep == 0)
    turn = jnp.where(last, chips, me_sp)

    def each(low, high, action):
        @pl.loop(low, high)
        def _(position):
            sp = jnp.where(position == chips, 0, position)
            for core in range(rep):

                @pl.when(position > 0 if core == 0 else position < chips)
                def _():
                    action(sp, core)

    def partners(action):
        @pl.when(me_sp > 0)
        def _():
            for core in range(1, rep):
                action(me_sp, (me_rep + core) % rep)

    def z_id(sp, core):
        return {"sp": sp, "rep": core}

    def x_id(s):
        return {"sub": s}

    def x_peer(j):
        s = me_x + j
        return jnp.where(s >= narrow, s - narrow, s)

    def signal(sem, where):
        pl.semaphore_signal(sem, inc=1, device_id=where, device_id_type=pl.DeviceIdType.MESH)

    def push(a, b, slot, where):
        pltpu.make_async_remote_copy(
            src_ref=a, dst_ref=b, send_sem=send.at[slot], recv_sem=recv.at[slot],
            device_id=where, device_id_type=pl.DeviceIdType.MESH,
        ).start()

    def drain(ref, sem):
        pltpu.make_async_copy(ref, ref, sem).wait()

    def rows(start, size):
        return pl.ds(pl.multiple_of(start, 8), size)

    barrier = pltpu.get_barrier_semaphore()

    @pl.loop(1, narrow)
    def _(j):
        signal(barrier, x_id(x_peer(j)))

    partners(lambda sp, core: signal(barrier, z_id(sp, core)))

    loads = [
        pltpu.make_async_copy(a, b, loaded.at[n]) for n, (a, b) in enumerate(zip(given, held))
    ]
    first = [0, where_is["fz_hi"], where_is["fz_lo"], where_is["gather"]]
    later = [n for n in range(count) if n not in first]
    for n in first + later:
        loads[n].start()
    def own_modes(waits):
        for n in waits:
            loads[n].wait()
        parts = [
            jnp.concatenate([field[128 * c + 32 * x : 128 * c + 32 * x + 32] for c in range(8)], 0)
            for x in range(4)
        ]
        main, packed = forward_z(parts, tabs)
        for c in range(8):
            b1[c, :32] = main[32 * c : 32 * c + 32]
            b1[c, 32:] = fold(packed[8 * c : 8 * c + 8])

    pl.when(turn == chips)(lambda: own_modes(first))

    before = jnp.where(turn == 0, 0, jnp.where(turn == 1, rep - 1, rep))
    pl.semaphore_wait(barrier, narrow - 1 + (rep - 1) * jnp.minimum(me_sp, 1) + before)

    @pl.when(turn < chips - 1)
    def _():
        for core in range(rep):
            signal(barrier, z_id(turn + 1, core))

    @pl.when(turn == chips - 1)
    def _():
        signal(barrier, z_id(0, 0))

    def send_field(sp, core):
        q = sp * rep + core
        push(src.at[rows(q * 32, 32)], fld.at[rows(me_z * 32, 32)], 1, z_id(sp, core))

    def spread_field():
        for y in range(32):
            src[32 * y : 32 * y + 32] = field[pl.ds(y, 32, stride=32)]
        each(0, turn, send_field)
        partners(send_field)

    def tell_before():
        each(0, turn, lambda sp, core: signal(ready.at[me_z], z_id(sp, core)))

    @pl.when(turn < chips)
    def _():
        tell_before()
        for n in first[:1]:
            loads[n].wait()
        pl.when(turn < chips - 1)(spread_field)
        own_modes(first[1:])

    for j in far_first(narrow):
        s = x_peer(j)
        push(b1.at[s], r1.at[me_x], 0, x_id(s))

    def send_modes(sp, core):
        q = sp * rep + core
        push(s3.at[q], n3.at[me_z], 3, z_id(sp, core))

    pl.when(turn == chips)(tell_before)
    pl.when(turn >= chips - 1)(spread_field)

    r1[me_x] = b1[me_x]
    fld[rows(me_z * 32, 32)] = src[rows(me_z * 32, 32)]
    for n in later:
        loads[n].wait()
    wts[...] = factor_weights(fac_x[...], fac_y[...], fac_z[...], channel, tabs)
    for full, hi, lo in ((mix, mix_hi, mix_lo), (w_in, *out[3:5]), (w_out, *out[5:7])):
        hi[...], lo[...] = split(full[...])
    for n, row in enumerate((gain, bias, b_in, b_out)):
        out[2][n] = jnp.broadcast_to(to_column(row[...]), (channels, 128))

    near = jnp.minimum(turn + 1 + AHEAD, chips + 1)

    def field_when_ready(sp, core):
        pl.semaphore_wait(ready.at[sp * rep + core], 1)
        send_field(sp, core)

    def both_when_ready(sp, core):
        pl.semaphore_wait(ready.at[sp * rep + core], 1)
        send_modes(sp, core)
        send_field(sp, core)

    each(turn + 1, near, field_when_ready)

    drain(r1.at[pl.ds(0, narrow - 1)], recv.at[0])
    blocks = [jnp.concatenate([r1[s, :32], unfold(r1[s, 32:])], 0) for s in range(8)]
    main, extra = spectral_filter(blocks, wts[...], tabs, lane_roll)
    for s in range(8):
        b2[s, :32] = main[s]
        b2[s, 32:] = fold(extra[s])

    for j in far_first(narrow):
        s = x_peer(j)
        push(b2.at[s], r2.at[me_x], 2, x_id(s))

    r2[me_x] = b2[me_x]
    drain(r2.at[pl.ds(0, narrow - 1)], recv.at[2])
    left = leftover_rows([unfold(r2[c, 32:]) for c in range(8)], lane_roll)
    for y in range(32):
        s3[y, :8] = r2[:, y]
        s3[y, 8:] = left[y : y + 1]

    @pl.when(near == chips + 1)
    def _():
        for step in far_first(chips):
            sp = me_sp + step
            for core in range(rep):
                send_modes(jnp.where(sp >= chips, sp - chips, sp), core)
        for core in range(1, rep):
            send_modes(me_sp, (me_rep + core) % rep)

    @pl.when(near < chips + 1)
    def _():
        each(0, turn, send_modes)
        partners(send_modes)
        each(turn + 1, near, send_modes)
        each(near, chips + 1, both_when_ready)

    n3[me_z] = s3[me_z]
    drain(n3.at[pl.ds(0, wide - 1)], recv.at[3])
    spectral = inverse_z(
        n3[:, :8].reshape(channels, 128), n3[:, 8:].reshape(wide, 128), (mix_hi[...], mix_lo[...]), tabs
    )
    drain(fld.at[pl.ds(0, 32 * (wide - 1))], recv.at[1])
    first = second = None
    for x in range(4):
        value = spectral[:, 128 * x : 128 * x + 128] + fld[pl.ds(x, channels, stride=4)]
        out[0][x] = value
        first = value if x == 0 else first + value
        second = value * value if x == 0 else second + value * value
    row = stats_row(group_partials(first), group_partials(second))
    st0[0] = row
    ar1[me_z] = row

    for step in far_first(chips):
        sp = me_sp + step
        sp = jnp.where(sp >= chips, sp - chips, sp)
        for core in range(rep):
            push(st0.at[0], ar1.at[me_z], 5, z_id(sp, core))
    for core in range(1, rep):
        push(st0.at[0], ar1.at[me_z], 5, z_id(me_sp, (me_rep + core) % rep))

    drain(ar1.at[pl.ds(0, wide - 1)], recv.at[5])
    row = jnp.sum(ar1[...].reshape(wide, 128), axis=0, keepdims=True)
    st1[0] = row
    ar2[me_x] = row

    for j in far_first(narrow):
        push(st1.at[0], ar2.at[me_x], 6, x_id(x_peer(j)))

    drain(ar2.at[pl.ds(0, narrow - 1)], recv.at[6])
    row = jnp.sum(ar2[...].reshape(narrow, 128), axis=0, keepdims=True)
    out[1][...] = row

    drain(b1.at[pl.ds(0, narrow - 1)], send.at[0])
    drain(src.at[pl.ds(0, 32 * (wide - 1))], send.at[1])
    drain(b2.at[pl.ds(0, narrow - 1)], send.at[2])
    drain(s3.at[pl.ds(0, wide - 1)], send.at[3])
    drain(ar1.at[pl.ds(0, wide - 1)], send.at[5])
    drain(ar2.at[pl.ds(0, narrow - 1)], send.at[6])


def channel_mlp(count, summed, stats, cols, in_hi, in_lo, out_hi, out_lo, out):
    channels = summed.shape[1]
    mean, inv = stats_columns(stats[...], count, channels)
    mean = jnp.broadcast_to(mean, (channels, 128))
    scale = jnp.broadcast_to(inv, (channels, 128)) * cols[0]
    wide_in, wide_out = (in_hi[...], in_lo[...]), (out_hi[...], out_lo[...])
    for x in range(summed.shape[0]):
        value = summed[x]
        normed = (value - mean) * scale + cols[1]
        hidden = gelu(dot3(wide_in, split(normed)) + cols[2])
        out[pl.ds(x, channels, stride=4)] = value + dot3(wide_out, split(hidden)) + cols[3]


def solution(mesh):
    shape = mesh.shape
    wide, narrow = shape["sp"] * shape["rep"], shape["sub"]
    replicated = P()
    placed = (P(("grp", "sp", "rep"), "sub", None, None),) + (replicated,) * 10

    def local(
        field, mix_weight, factor_x, factor_y, factor_z,
        norm_gain, norm_bias, w_in, b_in, w_out, b_out,
    ):
        held, x_local, ny, nz = field.shape
        channels = mix_weight.shape[0]
        nx = x_local * narrow
        kz = factor_z.shape[1]
        tables = build_tables(nx, ny, nz, kz, held, wide)
        sizes = dict(
            wide=wide, narrow=narrow, channels=channels, rep=shape["rep"],
            count=GROUP_CHANNELS * nx * ny * nz,
        )
        row = lambda v: v.reshape(1, -1)
        operands = [
            field.reshape(held * x_local * ny, nz), factor_x.T, factor_y.T, factor_z.T, mix_weight,
            row(norm_gain), row(norm_bias), w_in, row(b_in), w_out, row(b_out),
        ] + [jnp.asarray(tables[name]) for name in TABLES]
        cells = channels * x_local
        vmem = pl.BlockSpec(memory_space=pltpu.VMEM)
        f32 = lambda *dims: pltpu.VMEM(dims, F32)
        b16 = lambda *dims: pltpu.VMEM(dims, BF16)
        square = (channels, channels)
        handed = pl.pallas_call(
            lambda *refs: fused(sizes, *refs),
            out_shape=(
                jax.ShapeDtypeStruct((x_local, channels, nz), F32),
                jax.ShapeDtypeStruct((1, 128), F32),
                jax.ShapeDtypeStruct((4, channels, 128), F32),
            )
            + (jax.ShapeDtypeStruct(square, BF16),) * 4,
            in_specs=[pl.BlockSpec(memory_space=pltpu.HBM)] * len(operands),
            out_specs=(vmem,) * 7,
            scratch_shapes=[pltpu.VMEM(v.shape, v.dtype) for v in operands]
            + [pltpu.SemaphoreType.DMA((len(operands),))]
            + [
                f32(cells, nz), f32(cells, nz),
                f32(narrow, MSG, 128), f32(narrow, MSG, 128),
                f32(narrow, MSG, 128), f32(narrow, MSG, 128),
                f32(wide, 9, 128), f32(wide, 9, 128),
                f32(1, 1, 128), f32(wide, 1, 128), f32(1, 1, 128), f32(narrow, 1, 128),
                f32(ny, 9 * 128),
                b16(*square), b16(*square),
                pltpu.SemaphoreType.DMA((7,)), pltpu.SemaphoreType.DMA((7,)),
                pltpu.SemaphoreType.REGULAR((wide,)),
            ],
            compiler_params=pltpu.CompilerParams(
                collective_id=0, has_side_effects=True, vmem_limit_bytes=24 * 2**20
            ),
        )(*[pltpu.with_memory_space_constraint(v, pltpu.HBM) for v in operands])
        result = pl.pallas_call(
            functools.partial(channel_mlp, sizes["count"]),
            out_shape=jax.ShapeDtypeStruct((cells, nz), F32),
            in_specs=[vmem] * 7,
            out_specs=vmem,
            compiler_params=pltpu.CompilerParams(vmem_limit_bytes=24 * 2**20),
        )(*handed)
        return result.reshape(channels, x_local, 1, nz)

    return jax.shard_map(
        local,
        mesh=mesh,
        in_specs=placed,
        out_specs=P("grp", "sub", ("sp", "rep"), None),
        check_vma=False,
    )
```
